256 devices in a mesh: dp: 32 (over y_hi, z, core), tp: 8 (over x, y_lo).
Axes of the slice: x: 4, y: 4 (y_hi: 2, y_lo: 2; y = y_hi * 2 + y_lo), z: 8, core: 2. Of those that a mesh axis runs over, the one named last changes fastest.
Arguments:
- hidden: bfloat16 [32768, 4096], P(('dp', 'tp')), may hold values from -24 to 24
- query_grad: bfloat16 [32768, 4096], P('dp', 'tp'), may hold values from -1.5 to 1.5
- key_grad: bfloat16 [32768, 1024], P('dp', 'tp'), may hold values from -1.5 to 1.5
- value_grad: bfloat16 [32768, 1024], P('dp', 'tp'), may hold values from -1.5 to 1.5
- w_query: bfloat16 [4096, 4096], P(None, 'tp'), may hold values from -0.09375 to 0.09375
- w_key: bfloat16 [4096, 1024], P(None, 'tp'), may hold values from -0.09375 to 0.09375
- w_value: bfloat16 [4096, 1024], P(None, 'tp'), may hold values from -0.09375 to 0.09375
Outputs:
- hidden_grad: bfloat16 [32768, 4096], P(('dp', 'tp'))
- grad_query: float32 [4096, 4096], P('dp', 'tp')
- grad_key: float32 [4096, 1024], P('dp', 'tp')
- grad_value: float32 [4096, 1024], P('dp', 'tp')
The draws below stay inside these ranges and needn't reach their ends.
All inputs are finite; a program needn't handle non-finite values.
Results may differ from the reference program's by a relative error of at most 0.014.
Values may be sent and summed in bfloat16 or wider, within the bound.
A program may use at most 256 MiB of HBM per device.

```python
import jax
import jax.numpy as jnp
from jax import lax

D = 4096
HEAD = 128
Q_DEV = 4
KV_HEADS = 8
Q_W = 4096
KV_W = 1024
GROUP_TOK = 1024
TOKENS = 32768
N_DP = 32


def raised(entries, key, source, target, blocks, factor):
    owner, partner = [(jnp.arange(entries.shape[position]) // (entries.shape[position] // blocks)).reshape([-1 if axis == position else 1 for axis in range(entries.ndim)]) for position in (source, target)]
    chosen = jax.random.permutation(key, blocks)[partner]
    strong = (owner == chosen) | (owner == (partner + blocks // 2) % blocks)
    return jnp.where(strong, factor * entries, entries)


def steps_of(stream_key, shape, shards, low, largest):
    gain, own = 1.0, jax.random.fold_in(stream_key, 6)
    for dim, blocks in shards:
        draws = jnp.exp(jax.random.uniform(jax.random.fold_in(own, dim), (blocks,), jnp.float32, low / len(shards), largest / len(shards)))
        gain = gain * jnp.repeat(draws, shape[dim] // blocks).reshape([-1 if axis == dim else 1 for axis in range(len(shape))])
    return gain


def gaussian(key, dims, scale, most, pieces=(), dtype=jnp.bfloat16):
    result = scale * jax.random.normal(key, dims, jnp.float32)
    if pieces:
        result = result * steps_of(key, dims, pieces, -0.22, 0.18)
    return jnp.clip(result, -most, most).astype(dtype)


def noise_with(stream_key, extent, scale, most, split, heavy, kind=jnp.bfloat16):
    array = scale * jax.random.normal(stream_key, extent, jnp.float32)
    if split:
        array = array * steps_of(stream_key, extent, split, -0.22, 0.18)
    return jnp.clip(raised(array, jax.random.fold_in(stream_key, 3), *heavy), -most, most).astype(kind)


def setup_inputs(seed: int = 0) -> dict:
    key_of = jax.random.split(jax.random.key(seed), 8)
    return {
        "hidden": noise_with(key_of[0], (TOKENS, D), 1.0, 24.0, ((0, 256),), (0, 1, 256, 6.0)),
        "query_grad": gaussian(key_of[1], (TOKENS, Q_W), 0.25, 1.5, ((0, 32), (1, 8))),
        "key_grad": gaussian(key_of[2], (TOKENS, KV_W), 0.25, 1.5, ((0, 32), (1, 8))),
        "value_grad": gaussian(key_of[3], (TOKENS, KV_W), 0.25, 1.5, ((0, 32), (1, 8))),
        "w_query": gaussian(key_of[4], (D, Q_W), D ** -0.5, 0.09375, ((1, 8),)),
        "w_key": gaussian(key_of[5], (D, KV_W), D ** -0.5, 0.09375, ((1, 8),)),
        "w_value": gaussian(key_of[6], (D, KV_W), D ** -0.5, 0.09375, ((1, 8),)),
    }


def contract_rows(left, right):
    return lax.dot_general(left, right, (((0,), (0,)), ((), ())), preferred_element_type=jnp.float32)


def rounded(value):
    return lax.optimization_barrier(value.astype(jnp.bfloat16)).astype(jnp.float32)


def reference(hidden, query_grad, key_grad, value_grad, w_query, w_key, w_value):
    hidden_groups = hidden.reshape(N_DP, GROUP_TOK, D)
    query_groups = query_grad.reshape(N_DP, GROUP_TOK, Q_W)
    key_groups = key_grad.reshape(N_DP, GROUP_TOK, KV_W)
    value_groups = value_grad.reshape(N_DP, GROUP_TOK, KV_W)
    weight_heads = jnp.concatenate((w_query.reshape(D, KV_HEADS, Q_DEV * HEAD), w_key.reshape(D, KV_HEADS, HEAD), w_value.reshape(D, KV_HEADS, HEAD)), axis=2).astype(jnp.float32)

    def one_group(totals, inputs):
        grad_wq, grad_wk, grad_wv = totals
        hid, qgr, kgr, vgr = inputs
        grad_heads = jnp.concatenate((qgr.reshape(GROUP_TOK, KV_HEADS, Q_DEV * HEAD), kgr.reshape(GROUP_TOK, KV_HEADS, HEAD), vgr.reshape(GROUP_TOK, KV_HEADS, HEAD)), axis=2).astype(jnp.float32)
        parts = jnp.einsum("thc,dhc->htd", grad_heads, weight_heads)
        hid_grad = jnp.sum(rounded(parts), axis=0).astype(jnp.bfloat16)
        grad_wq = grad_wq + rounded(contract_rows(hid, qgr))
        grad_wk = grad_wk + rounded(contract_rows(hid, kgr))
        grad_wv = grad_wv + rounded(contract_rows(hid, vgr))
        return (grad_wq, grad_wk, grad_wv), hid_grad

    zeros = (jnp.zeros((D, Q_W), jnp.float32), jnp.zeros((D, KV_W), jnp.float32), jnp.zeros((D, KV_W), jnp.float32))
    totals, outputs = lax.scan(one_group, zeros, (hidden_groups, query_groups, key_groups, value_groups))
    hidden_grad = outputs.reshape(TOKENS, D)
    return hidden_grad, totals[0], totals[1], totals[2]
```

```python
import jax
import jax.numpy as jnp
from jax import lax
from jax.experimental import pallas as pl
from jax.experimental.pallas import tpu as pltpu
from jax.sharding import PartitionSpec as P

MESH = pl.DeviceIdType.MESH
BF16 = jnp.bfloat16
F32 = jnp.float32
T = 128
D = 4096
H = 2048
HH = 1024
CQ = 512
CK = 128
C = 768


def nt(left, right):
    return lax.dot_general(left, right, (((1,), (1,)), ((), ())), preferred_element_type=F32)


def tn(left, right):
    return lax.dot_general(left, right, (((0,), (0,)), ((), ())), preferred_element_type=F32)


def kernel(
    hidden_ref,
    q_ref,
    k_ref,
    v_ref,
    wq_ref,
    wk_ref,
    wv_ref,
    out_ref,
    gq_ref,
    gk_ref,
    gv_ref,
    hid,
    hsend,
    gown,
    goth,
    wmine,
    woth,
    wsend,
    hg,
    wg,
    ccs,
    ccr,
    xs,
    xr,
    zs,
    zr,
    fin,
    yr,
    yos,
    yor,
    lsem,
    ssem,
    rsem,
    yssem,
    yrsem,
):
    dp = lax.axis_index("dp")
    tp = lax.axis_index("tp")
    c = lax.rem(dp, 2)
    z = lax.rem(dp // 2, 8)
    yh = dp // 16
    yl = lax.rem(tp, 2)
    x = tp // 2
    e = lax.rem(z, 2)

    def dev(xx=None, yhh=None, yll=None, zz=None, cc=None):
        xx = x if xx is None else xx
        yhh = yh if yhh is None else yhh
        yll = yl if yll is None else yll
        zz = z if zz is None else zz
        cc = c if cc is None else cc
        return (yhh * 16 + zz * 2 + cc, xx * 2 + yll)

    XP = dev(xx=lax.rem(x + 1, 4))
    XM = dev(xx=lax.rem(x + 3, 4))
    YI = dev(yll=1 - yl)
    YO = dev(yhh=1 - yh, yll=1 - yl)
    Y2 = dev(yhh=1 - yh)
    ZP = dev(zz=lax.rem(z + 1, 8))
    ZM = dev(zz=lax.rem(z + 7, 8))
    ZX = dev(zz=z + 1 - 2 * e)
    CC = dev(cc=1 - c)

    counter = [0]
    sent = []

    def remote(src, dst, target, send=None, recv=None):
        if send is None:
            i = counter[0]
            counter[0] += 1
            send, recv = ssem.at[i], rsem.at[i]
        copy = pltpu.make_async_remote_copy(
            src_ref=src, dst_ref=dst, send_sem=send, recv_sem=recv, device_id=target, device_id_type=MESH
        )
        return copy

    def start(copy):
        copy.start()
        sent.append(copy)

    def local(src, dst, i):
        copy = pltpu.make_async_copy(src, dst, lsem.at[i])
        copy.start()
        return copy

    mine = pl.ds(pl.multiple_of(yl * H, H), H)
    other = pl.ds(pl.multiple_of((1 - yl) * H, H), H)
    load_a = local(hidden_ref.at[:, mine], hid.at[pl.ds(0, T)], 0)
    load_b = local(hidden_ref.at[:, other], hsend, 1)
    wrow = c * 1024 + e * 512
    wrows = pl.ds(pl.multiple_of((1 - yl) * H + wrow, 512), 512)
    local(wq_ref.at[wrows], wsend.at[:, pl.ds(0, CQ)], 2)
    local(wk_ref.at[wrows], wsend.at[:, pl.ds(CQ, CK)], 2)
    local(wv_ref.at[wrows], wsend.at[:, pl.ds(CQ + CK, CK)], 2)
    for r, off in enumerate((0, 1, 3, 2)):
        for s in range(2):
            block = lax.rem(x + off, 4) * 2 + (yl if s == 0 else 1 - yl)
            src = pl.ds(pl.multiple_of(block * T, T), T)
            dst = pl.ds(r * 256 + s * T, T)
            local(q_ref.at[src], gown.at[dst, pl.ds(0, CQ)], 3)
            local(k_ref.at[src], gown.at[dst, pl.ds(CQ, CK)], 3)
            local(v_ref.at[src], gown.at[dst, pl.ds(CQ + CK, CK)], 3)
    local(wq_ref.at[mine], wmine.at[:, pl.ds(0, CQ)], 4)
    local(wk_ref.at[mine], wmine.at[:, pl.ds(CQ, CK)], 4)
    local(wv_ref.at[mine], wmine.at[:, pl.ds(CQ + CK, CK)], 4)

    def wait_local(buffer, i):
        pltpu.make_async_copy(buffer, buffer, lsem.at[i]).wait()

    barrier = pltpu.get_barrier_semaphore()
    for target in (XP, XM, YI, YO, Y2, ZP, ZM, CC):
        pl.semaphore_signal(barrier, inc=1, device_id=target, device_id_type=MESH)
    pl.semaphore_wait(barrier, 8)

    def rows(r, s, half=None):
        first = r * 256 + s * T
        return pl.ds(first, T) if half is None else pl.ds(first + half * 64, 64)

    a_p = [remote(hid.at[rows(0, 0, i)], hid.at[rows(2, 0, i)], XP) for i in range(2)]
    a_m = [remote(hid.at[rows(0, 0, i)], hid.at[rows(1, 0, i)], XM) for i in range(2)]
    b_y = [remote(hsend.at[pl.ds(64 * i, 64)], hid.at[rows(0, 1, i)], YI) for i in range(2)]
    b_p = [remote(hid.at[rows(0, 1, i)], hid.at[rows(2, 1, i)], XP) for i in range(2)]
    b_m = [remote(hid.at[rows(0, 1, i)], hid.at[rows(1, 1, i)], XM) for i in range(2)]
    f_p = [remote(hid.at[rows(2, s, 0)], hid.at[rows(3, s, 0)], XP) for s in range(2)]
    f_m = [remote(hid.at[rows(1, s, 1)], hid.at[rows(3, s, 1)], XM) for s in range(2)]
    g_y = {
        (r, s): remote(gown.at[rows(r, s)], goth.at[rows(r, 1 - s)], YI) for r in (3, 1, 2, 0) for s in range(2)
    }

    def wpiece(cc, ee, k):
        return pl.ds(pl.multiple_of(cc * 1024 + ee * 512 + k * 256, 256), 256)

    w_y = [remote(wsend.at[pl.ds(256 * k, 256)], woth.at[wpiece(c, e, k)], YO) for k in range(2)]
    w_z = [remote(woth.at[wpiece(c, e, k)], woth.at[wpiece(c, e, k)], ZX) for k in range(2)]
    w_c = [remote(woth.at[wpiece(c, e, k)], woth.at[wpiece(c, e, k)], CC) for k in range(2)]
    w_d = [remote(woth.at[wpiece(c, 1 - e, k)], woth.at[wpiece(c, 1 - e, k)], CC) for k in range(2)]
    xc = {
        (d, b, s): remote(xs.at[d, b, s], xr.at[d, b, s], XP if d == 0 else XM)
        for d in range(2)
        for b in range(3)
        for s in range(2)
    }
    o_y = remote(yos, yor, YI)
    cc_copy = [remote(ccs.at[n], ccr.at[n], CC) for n in range(2)]
    steps = (pl.ds(0, 64), pl.ds(64, 128), pl.ds(192, 128), pl.ds(320, 128))
    zc = {
        (n, d, i): remote(zs.at[n, d, steps[i]], zr.at[n, d, steps[i]], ZP if d == 0 else ZM)
        for n in range(2)
        for d in range(2)
        for i in range(4)
    }

    load_a.wait()
    for i in range(2):
        start(a_p[i])
        start(a_m[1 - i])
    load_b.wait()
    for i in range(2):
        start(b_y[i])
    wait_local(wsend, 2)
    for k in range(2):
        start(w_y[k])
    wait_local(gown, 3)
    for r in (3, 1, 2, 0):
        for s in (0, 1):
            start(g_y[r, s])
    wait_local(wmine, 4)

    def hg_own():
        def step(n, carry):
            cols = pl.ds(pl.multiple_of(n * 256, 256), 256)
            w = wmine[cols, :]
            for m in range(2):
                hg[pl.ds(m * 512, 512), cols] = nt(gown[pl.ds(m * 512, 512), :], w)
            return carry

        lax.fori_loop(0, 8, step, 0)

    def hg_other(r):
        def step(n, carry):
            cols = pl.ds(pl.multiple_of(n * 256, 256), 256)
            hg[pl.ds(r * 256, 256), cols] += nt(goth[pl.ds(r * 256, 256), :], woth[cols, :])
            return carry

        lax.fori_loop(0, 8, step, 0)

    def wg_add(n, g, first, depth, fresh):
        def step(m, carry):
            cols = pl.ds(pl.multiple_of(m * 512, 512), 512)
            part = tn(hid[pl.ds(first, depth), cols], g[pl.ds(first, depth), :])
            if fresh:
                wg[n, cols, :] = part
            else:
                wg[n, cols, :] += part
            return carry

        lax.fori_loop(0, 4, step, 0)

    def cc_send(n):
        def step(zz, carry):
            src = pl.ds(pl.multiple_of((2 * zz + 1 - c) * T, T), T)
            dst = pl.ds(pl.multiple_of(zz * T, T), T)
            ccs[n, dst, :] = wg[n, src, :].astype(BF16)
            return carry

        lax.fori_loop(0, 8, step, 0)
        start(cc_copy[n])

    def pair_sum(n, zz, first=0, size=T):
        src = pl.ds(pl.multiple_of((2 * zz + c) * T + first, size), size)
        dst = pl.ds(pl.multiple_of(zz * T + first, size), size)
        return wg[n, src, :] + ccr[n, dst, :].astype(F32)

    def z_step(n, i):
        if i == 0:
            far = lax.rem(z + 4, 8)
            zs[n, 0, steps[0], :] = pair_sum(n, far, 0, 64).astype(BF16)
            zs[n, 1, steps[0], :] = pair_sum(n, far, 64, 64).astype(BF16)
        else:
            for d in range(2):
                zz = lax.rem(z + 4 - i, 8) if d == 0 else lax.rem(z + 4 + i, 8)
                zc[n, d, i - 1].wait_recv()
                if i == 1:
                    for half in range(2):
                        part = pair_sum(n, zz, half * 64, 64)
                        if half == d:
                            part = part + zr[n, d, steps[0], :].astype(F32)
                        zs[n, d, pl.ds(64 + half * 64, 64), :] = part.astype(BF16)
                else:
                    part = pair_sum(n, zz) + zr[n, d, steps[i - 1], :].astype(F32)
                    zs[n, d, steps[i], :] = part.astype(BF16)
                start(zc[n, d, i])
        if i == 0:
            for d in range(2):
                start(zc[n, d, 0])

    def z_last(n):
        for d in range(2):
            zc[n, d, 3].wait_recv()
        total = pair_sum(n, z) + zr[n, 0, steps[3], :].astype(F32) + zr[n, 1, steps[3], :].astype(F32)
        fin[n] = total.astype(BF16)

    left, right = pl.ds(0, HH), pl.ds(HH, HH)

    def x_far():
        for s in (1, 0):
            block = pl.ds(3 * 256 + s * T, T)
            xs[0, 0, s] = hg[block, left].astype(BF16)
            start(xc[0, 0, s])
            xs[1, 0, s] = hg[block, right].astype(BF16)
            start(xc[1, 0, s])

    def x_direct(s):
        xs[0, 1, s] = hg[pl.ds(1 * 256 + s * T, T), right].astype(BF16)
        start(xc[0, 1, s])
        xs[1, 1, s] = hg[pl.ds(2 * 256 + s * T, T), left].astype(BF16)
        start(xc[1, 1, s])

    def x_summed(s):
        xc[0, 0, s].wait_recv()
        xs[0, 2, s] = (hg[pl.ds(1 * 256 + s * T, T), left] + xr[0, 0, s].astype(F32)).astype(BF16)
        start(xc[0, 2, s])
        xc[1, 0, s].wait_recv()
        xs[1, 2, s] = (hg[pl.ds(2 * 256 + s * T, T), right] + xr[1, 0, s].astype(F32)).astype(BF16)
        start(xc[1, 2, s])

    def x_total(s):
        for d in range(2):
            xc[d, 1, s].wait_recv()
            xc[d, 2, s].wait_recv()
        block = pl.ds(s * T, T)
        lo = hg[block, left] + xr[0, 2, s].astype(F32) + xr[1, 1, s].astype(F32)
        hi = hg[block, right] + xr[0, 1, s].astype(F32) + xr[1, 2, s].astype(F32)
        return lo.astype(BF16), hi.astype(BF16)

    hg_own()
    a_p[0].wait_recv()
    start(f_p[0])
    a_m[1].wait_recv()
    start(f_m[0])
    w_y[0].wait_recv()
    start(w_z[0])
    start(w_c[0])
    for i in range(2):
        b_y[i].wait_recv()
    for i in range(2):
        start(b_p[i])
        start(b_m[1 - i])
    w_y[1].wait_recv()
    start(w_z[1])
    start(w_c[1])
    w_z[0].wait_recv()
    start(w_d[0])
    b_p[0].wait_recv()
    start(f_p[1])
    b_m[1].wait_recv()
    start(f_m[1])
    w_z[1].wait_recv()
    start(w_d[1])
    a_p[1].wait_recv()
    a_m[0].wait_recv()
    b_p[1].wait_recv()
    b_m[0].wait_recv()
    wg_add(0, gown, 0, 768, True)
    for k in range(2):
        w_c[k].wait_recv()
        w_d[k].wait_recv()
    g_y[3, 0].wait_recv()
    g_y[3, 1].wait_recv()
    hg_other(3)
    x_far()
    for s in range(2):
        f_p[s].wait_recv()
        f_m[s].wait_recv()
    wg_add(0, gown, 768, 256, False)
    cc_send(0)
    for r in (1, 2):
        g_y[r, 0].wait_recv()
        g_y[r, 1].wait_recv()
        hg_other(r)
    x_direct(1)
    cc_copy[0].wait_recv()
    z_step(0, 0)
    x_summed(1)
    x_direct(0)
    z_step(0, 1)
    g_y[0, 0].wait_recv()
    g_y[0, 1].wait_recv()
    wg_add(1, goth, 0, 1024, True)
    cc_send(1)
    x_summed(0)
    hg_other(0)
    cc_copy[1].wait_recv()
    z_step(1, 0)
    z_step(0, 2)
    z_step(1, 1)
    lo, hi = x_total(1)
    yos[:, left] = lo
    yos[:, right] = hi
    start(o_y)
    z_step(0, 3)
    z_step(1, 2)
    z_last(0)

    own_copy = remote(fin.at[0], yr.at[yh], dev(yhh=yl), yssem.at[0], yrsem.at[yh])
    other_copy = remote(fin.at[1], yr.at[yh], dev(yhh=yl, yll=1 - yl), yssem.at[1], yrsem.at[yh])

    @pl.when(yh != yl)
    def _():
        own_copy.start()

    z_step(1, 3)
    lo, hi = x_total(0)
    out_ref[:, pl.ds(pl.multiple_of(yl * H, H), HH)] = lo
    out_ref[:, pl.ds(pl.multiple_of(yl * H + HH, HH), HH)] = hi
    o_y.wait_recv()
    out_ref[:, pl.ds(pl.multiple_of((1 - yl) * H, H), H)] = yor[...]
    z_last(1)
    other_copy.start()

    def finish(total):
        gq_ref[...] = total[:, :CQ]
        gk_ref[...] = total[:, CQ : CQ + CK]
        gv_ref[...] = total[:, CQ + CK :]

    def arrived(slot):
        pltpu.make_async_copy(yr.at[slot], yr.at[slot], yrsem.at[slot]).wait()

    @pl.when(yh == yl)
    def _():
        arrived(1 - yh)
        finish(fin[0].astype(F32) + yr[1 - yh].astype(F32))

    @pl.when(yh != yl)
    def _():
        arrived(0)
        arrived(1)
        finish(yr[0].astype(F32) + yr[1].astype(F32))
        own_copy.wait_send()

    other_copy.wait_send()
    for copy in sent:
        copy.wait_send()


N_SEM = 80


def local_step(*args):
    vmem = pl.BlockSpec(memory_space=pltpu.VMEM)
    scratch = [
        pltpu.VMEM((1024, H), BF16),
        pltpu.VMEM((T, H), BF16),
        pltpu.VMEM((1024, C), BF16),
        pltpu.VMEM((1024, C), BF16),
        pltpu.VMEM((H, C), BF16),
        pltpu.VMEM((H, C), BF16),
        pltpu.VMEM((512, C), BF16),
        pltpu.VMEM((1024, H), F32),
        pltpu.VMEM((2, H, C), F32),
        pltpu.VMEM((2, 1024, C), BF16),
        pltpu.VMEM((2, 1024, C), BF16),
        pltpu.VMEM((2, 3, 2, T, HH), BF16),
        pltpu.VMEM((2, 3, 2, T, HH), BF16),
        pltpu.VMEM((2, 2, 448, C), BF16),
        pltpu.VMEM((2, 2, 448, C), BF16),
        pltpu.VMEM((2, T, C), BF16),
        pltpu.VMEM((2, T, C), BF16),
        pltpu.VMEM((T, H), BF16),
        pltpu.VMEM((T, H), BF16),
        pltpu.SemaphoreType.DMA((5,)),
        pltpu.SemaphoreType.DMA((N_SEM,)),
        pltpu.SemaphoreType.DMA((N_SEM,)),
        pltpu.SemaphoreType.DMA((2,)),
        pltpu.SemaphoreType.DMA((2,)),
    ]
    return pl.pallas_call(
        kernel,
        out_shape=(
            jax.ShapeDtypeStruct((T, D), BF16),
            jax.ShapeDtypeStruct((T, CQ), F32),
            jax.ShapeDtypeStruct((T, CK), F32),
            jax.ShapeDtypeStruct((T, CK), F32),
        ),
        in_specs=[pl.BlockSpec(memory_space=pl.ANY)] * 7,
        out_specs=(vmem, vmem, vmem, vmem),
        scratch_shapes=scratch,
        compiler_params=pltpu.CompilerParams(
            collective_id=0, has_side_effects=True, vmem_limit_bytes=67043328
        ),
    )(*args)


def solution(mesh):
    both = P(("dp", "tp"), None)
    split = P("dp", "tp")
    return jax.shard_map(
        local_step,
        mesh=mesh,
        in_specs=(both, split, split, split, P(None, "tp"), P(None, "tp"), P(None, "tp")),
        out_specs=(both, split, split, split),
        check_vma=False,
    )
```

```python
import jax
import jax.numpy as jnp
from jax import lax
from jax.experimental import pallas as pl
from jax.experimental.pallas import tpu as pltpu
from jax.sharding import PartitionSpec as P

MESH = pl.DeviceIdType.MESH
BF16 = jnp.bfloat16
F32 = jnp.float32
T = 128
D = 4096
H = 2048
HH = 1024
CQ = 512
CK = 128
C = 768
CW = 384


def nt(left, right):
    return lax.dot_general(left, right, (((1,), (1,)), ((), ())), preferred_element_type=F32)


def tn(left, right):
    return lax.dot_general(left, right, (((0,), (0,)), ((), ())), preferred_element_type=F32)


def kernel(
    hidden_ref,
    q_ref,
    k_ref,
    v_ref,
    wq_ref,
    wk_ref,
    wv_ref,
    out_ref,
    gq_ref,
    gk_ref,
    gv_ref,
    hid,
    hsend,
    gown,
    goth,
    wmine,
    woth,
    wt,
    wsend,
    hg,
    wg,
    ccs,
    ccr,
    xs,
    xr,
    zs,
    zr,
    fin,
    yr,
    yos,
    yor,
    os,
    gs,
    lsem,
    ssem,
    rsem,
    yssem,
    yrsem,
):
    dp = lax.axis_index("dp")
    tp = lax.axis_index("tp")
    c = lax.rem(dp, 2)
    z = lax.rem(dp // 2, 8)
    yh = dp // 16
    yl = lax.rem(tp, 2)
    x = tp // 2
    e = lax.rem(z, 2)

    def dev(xx=None, yhh=None, yll=None, zz=None, cc=None):
        xx = x if xx is None else xx
        yhh = yh if yhh is None else yhh
        yll = yl if yll is None else yll
        zz = z if zz is None else zz
        cc = c if cc is None else cc
        return (yhh * 16 + zz * 2 + cc, xx * 2 + yll)

    XP = dev(xx=lax.rem(x + 1, 4))
    XM = dev(xx=lax.rem(x + 3, 4))
    YI = dev(yll=1 - yl)
    YO = dev(yhh=1 - yh, yll=1 - yl)
    Y2 = dev(yhh=1 - yh)
    ZP = dev(zz=lax.rem(z + 1, 8))
    ZM = dev(zz=lax.rem(z + 7, 8))
    ZX = dev(zz=z + 1 - 2 * e)
    CC = dev(cc=1 - c)

    counter = [0]
    sent = []

    def remote(src, dst, target, send=None, recv=None):
        if send is None:
            i = counter[0]
            counter[0] += 1
            send, recv = ssem.at[i], rsem.at[i]
        copy = pltpu.make_async_remote_copy(
            src_ref=src, dst_ref=dst, send_sem=send, recv_sem=recv, device_id=target, device_id_type=MESH
        )
        return copy

    def start(copy):
        copy.start()
        sent.append(copy)

    def local(src, dst, i):
        copy = pltpu.make_async_copy(src, dst, lsem.at[i])
        copy.start()
        return copy

    mine = pl.ds(pl.multiple_of(yl * H, H), H)
    other = pl.ds(pl.multiple_of((1 - yl) * H, H), H)
    load_a = local(hidden_ref.at[:, mine], hid.at[pl.ds(0, T)], 0)
    load_b = local(hidden_ref.at[:, other], hsend, 1)
    wrow = c * 1024 + e * 512
    wrows = pl.ds(pl.multiple_of((1 - yl) * H + wrow, 512), 512)
    local(wq_ref.at[wrows], wsend.at[:, pl.ds(0, CQ)], 2)
    local(wk_ref.at[wrows], wsend.at[:, pl.ds(CQ, CK)], 2)
    local(wv_ref.at[wrows], wsend.at[:, pl.ds(CQ + CK, CK)], 2)
    for r, off in enumerate((0, 1, 3, 2)):
        for s in range(2):
            block = lax.rem(x + off, 4) * 2 + (yl if s == 0 else 1 - yl)
            src = pl.ds(pl.multiple_of(block * T, T), T)
            dst = pl.ds(r * 256 + s * T, T)
            local(q_ref.at[src], gown.at[dst, pl.ds(0, CQ)], 3)
            local(k_ref.at[src], gown.at[dst, pl.ds(CQ, CK)], 3)
            local(v_ref.at[src], gown.at[dst, pl.ds(CQ + CK, CK)], 3)
    local(wq_ref.at[mine], wmine.at[:, pl.ds(0, CQ)], 4)
    local(wk_ref.at[mine], wmine.at[:, pl.ds(CQ, CK)], 4)
    local(wv_ref.at[mine], wmine.at[:, pl.ds(CQ + CK, CK)], 4)

    def wait_local(buffer, i):
        pltpu.make_async_copy(buffer, buffer, lsem.at[i]).wait()

    barrier = pltpu.get_barrier_semaphore()
    for target in (XP, XM, YI, YO, Y2, ZP, ZM, CC):
        pl.semaphore_signal(barrier, inc=1, device_id=target, device_id_type=MESH)
    pl.semaphore_wait(barrier, 8)

    def rows(r, s, half=None):
        first = r * 256 + s * T
        return pl.ds(first, T) if half is None else pl.ds(first + half * 64, 64)

    a_p = [remote(hid.at[rows(0, 0, i)], hid.at[rows(2, 0, i)], XP) for i in range(2)]
    a_m = [remote(hid.at[rows(0, 0, i)], hid.at[rows(1, 0, i)], XM) for i in range(2)]
    b_y = [remote(hsend.at[pl.ds(64 * i, 64)], hid.at[rows(0, 1, i)], YI) for i in range(2)]
    b_p = [remote(hid.at[rows(0, 1, i)], hid.at[rows(2, 1, i)], XP) for i in range(2)]
    b_m = [remote(hid.at[rows(0, 1, i)], hid.at[rows(1, 1, i)], XM) for i in range(2)]
    f_p = [remote(hid.at[rows(2, s, 0)], hid.at[rows(3, s, 0)], XP) for s in range(2)]
    f_m = [remote(hid.at[rows(1, s, 1)], hid.at[rows(3, s, 1)], XM) for s in range(2)]
    g_y = {
        (r, s): remote(gown.at[rows(r, s)], goth.at[rows(r, 1 - s)], YI) for r in (3, 1, 2, 0) for s in range(2)
    }

    def wpiece(cc, ee, k):
        return pl.ds(pl.multiple_of(cc * 1024 + ee * 512 + k * 256, 256), 256)

    w_y = [remote(wsend.at[pl.ds(256 * k, 256)], woth.at[wpiece(c, e, k)], YO) for k in range(2)]
    w_z = [remote(woth.at[wpiece(c, e, k)], woth.at[wpiece(c, e, k)], ZX) for k in range(2)]
    w_c = [remote(woth.at[wpiece(c, e, k)], woth.at[wpiece(c, e, k)], CC) for k in range(2)]
    w_d = [remote(woth.at[wpiece(c, 1 - e, k)], woth.at[wpiece(c, 1 - e, k)], CC) for k in range(2)]
    xc = {
        (d, b, s): remote(xs.at[d, b, s], xr.at[d, b, s], XP if d == 0 else XM)
        for d in range(2)
        for b in range(3)
        for s in range(2)
    }
    o_y = remote(yos, yor, YI)
    cc_copy = [remote(ccs.at[n], ccr.at[n], CC) for n in range(4)]
    steps = (pl.ds(0, 64), pl.ds(64, 128), pl.ds(192, 128), pl.ds(320, 128))
    zc = {
        (n, d, i): remote(zs.at[n, d, steps[i]], zr.at[n, d, steps[i]], ZP if d == 0 else ZM)
        for n in range(4)
        for d in range(2)
        for i in range(4)
    }

    load_a.wait()
    for i in range(2):
        start(a_p[i])
        start(a_m[1 - i])
    load_b.wait()
    for i in range(2):
        start(b_y[i])
    wait_local(wsend, 2)
    for k in range(2):
        start(w_y[k])
    wait_local(gown, 3)
    for r in (3, 1, 2, 0):
        for s in (0, 1):
            start(g_y[r, s])
    wait_local(wmine, 4)

    def hg_own():
        def step(n, carry):
            cols = pl.ds(pl.multiple_of(n * 256, 256), 256)
            w = wmine[cols, :]
            for m in range(2):
                hg[pl.ds(m * 512, 512), cols] = nt(gown[pl.ds(m * 512, 512), :], w)
            return carry

        lax.fori_loop(0, 8, step, 0)

    def turn(cc, ee, k):
        piece = wpiece(cc, ee, k)
        wt[:, piece] = woth[piece, :].T

    def hg_other(r):
        def step(n, carry):
            cols = pl.ds(pl.multiple_of(n * 512, 512), 512)
            block = pl.ds(r * 256, 256)
            hg[block, cols] += jnp.dot(goth[block, :], wt[:, cols], preferred_element_type=F32)
            return carry

        lax.fori_loop(0, 4, step, 0)

    def wg_add(n, first, depth, fresh):
        g = gown if n < 2 else goth
        part_cols = pl.ds((n % 2) * CW, CW)

        def step(m, carry):
            cols = pl.ds(pl.multiple_of(m * 512, 512), 512)
            part = tn(hid[pl.ds(first, depth), cols], g[pl.ds(first, depth), part_cols])
            if fresh:
                wg[n, cols, :] = part
            else:
                wg[n, cols, :] += part
            return carry

        lax.fori_loop(0, 4, step, 0)

    def cc_send(n):
        def step(zz, carry):
            src = pl.ds(pl.multiple_of((2 * zz + 1 - c) * T, T), T)
            dst = pl.ds(pl.multiple_of(zz * T, T), T)
            ccs[n, dst, :] = wg[n, src, :].astype(BF16)
            return carry

        lax.fori_loop(0, 8, step, 0)
        start(cc_copy[n])

    def pair_sum(n, zz, first=0, size=T):
        src = pl.ds(pl.multiple_of((2 * zz + c) * T + first, size), size)
        dst = pl.ds(pl.multiple_of(zz * T + first, size), size)
        return wg[n, src, :] + ccr[n, dst, :].astype(F32)

    def z_step(n, i):
        if i == 0:
            far = lax.rem(z + 4, 8)
            zs[n, 0, steps[0], :] = pair_sum(n, far, 0, 64).astype(BF16)
            zs[n, 1, steps[0], :] = pair_sum(n, far, 64, 64).astype(BF16)
        else:
            for d in range(2):
                zz = lax.rem(z + 4 - i, 8) if d == 0 else lax.rem(z + 4 + i, 8)
                zc[n, d, i - 1].wait_recv()
                if i == 1:
                    for half in range(2):
                        part = pair_sum(n, zz, half * 64, 64)
                        if half == d:
                            part = part + zr[n, d, steps[0], :].astype(F32)
                        zs[n, d, pl.ds(64 + half * 64, 64), :] = part.astype(BF16)
                else:
                    part = pair_sum(n, zz) + zr[n, d, steps[i - 1], :].astype(F32)
                    zs[n, d, steps[i], :] = part.astype(BF16)
                start(zc[n, d, i])
        if i == 0:
            for d in range(2):
                start(zc[n, d, 0])

    def z_last(n):
        for d in range(2):
            zc[n, d, 3].wait_recv()
        total = pair_sum(n, z) + zr[n, 0, steps[3], :].astype(F32) + zr[n, 1, steps[3], :].astype(F32)
        fin[n] = total.astype(BF16)

    left, right = pl.ds(0, HH), pl.ds(HH, HH)

    def x_far():
        for s in (1, 0):
            block = pl.ds(3 * 256 + s * T, T)
            xs[0, 0, s] = hg[block, left].astype(BF16)
            start(xc[0, 0, s])
            xs[1, 0, s] = hg[block, right].astype(BF16)
            start(xc[1, 0, s])

    def x_direct(s):
        xs[0, 1, s] = hg[pl.ds(1 * 256 + s * T, T), right].astype(BF16)
        start(xc[0, 1, s])
        xs[1, 1, s] = hg[pl.ds(2 * 256 + s * T, T), left].astype(BF16)
        start(xc[1, 1, s])

    def x_summed(s):
        xc[0, 0, s].wait_recv()
        xs[0, 2, s] = (hg[pl.ds(1 * 256 + s * T, T), left] + xr[0, 0, s].astype(F32)).astype(BF16)
        start(xc[0, 2, s])
        xc[1, 0, s].wait_recv()
        xs[1, 2, s] = (hg[pl.ds(2 * 256 + s * T, T), right] + xr[1, 0, s].astype(F32)).astype(BF16)
        start(xc[1, 2, s])

    def x_total(s):
        for d in range(2):
            xc[d, 1, s].wait_recv()
            xc[d, 2, s].wait_recv()
        block = pl.ds(s * T, T)
        lo = hg[block, left] + xr[0, 2, s].astype(F32) + xr[1, 1, s].astype(F32)
        hi = hg[block, right] + xr[0, 1, s].astype(F32) + xr[1, 2, s].astype(F32)
        return lo.astype(BF16), hi.astype(BF16)

    def send_fin(n):
        if n < 2:

            @pl.when(yh != yl)
            def _():
                last[n].start()
        else:
            last[n].start()

    last = [
        remote(
            fin.at[n],
            yr.at[yh, n % 2],
            dev(yhh=yl) if n < 2 else dev(yhh=yl, yll=1 - yl),
            yssem.at[n],
            yrsem.at[yh, n % 2],
        )
        for n in range(4)
    ]

    hg_own()
    a_p[0].wait_recv()
    start(f_p[0])
    a_m[1].wait_recv()
    start(f_m[0])
    w_y[0].wait_recv()
    start(w_z[0])
    start(w_c[0])
    for i in range(2):
        b_y[i].wait_recv()
    for i in range(2):
        start(b_p[i])
        start(b_m[1 - i])
    turn(c, e, 0)
    wg_add(0, 0, 256, True)
    wg_add(1, 0, 256, True)
    w_c[0].wait_recv()
    turn(1 - c, e, 0)
    w_y[1].wait_recv()
    start(w_z[1])
    start(w_c[1])
    w_z[0].wait_recv()
    start(w_d[0])
    turn(c, e, 1)
    turn(c, 1 - e, 0)
    b_p[0].wait_recv()
    start(f_p[1])
    b_m[1].wait_recv()
    start(f_m[1])
    w_c[1].wait_recv()
    turn(1 - c, e, 1)
    w_d[0].wait_recv()
    turn(1 - c, 1 - e, 0)
    w_z[1].wait_recv()
    start(w_d[1])
    turn(c, 1 - e, 1)
    w_d[1].wait_recv()
    turn(1 - c, 1 - e, 1)
    g_y[3, 0].wait_recv()
    g_y[3, 1].wait_recv()
    hg_other(3)
    x_far()
    a_p[1].wait_recv()
    a_m[0].wait_recv()
    b_p[1].wait_recv()
    b_m[0].wait_recv()
    wg_add(0, 256, 512, False)
    wg_add(1, 256, 512, False)
    for s in range(2):
        f_p[s].wait_recv()
        f_m[s].wait_recv()
    wg_add(0, 768, 256, False)
    cc_send(0)
    wg_add(1, 768, 256, False)
    cc_send(1)
    g_y[1, 0].wait_recv()
    g_y[1, 1].wait_recv()
    hg_other(1)
    cc_copy[0].wait_recv()
    z_step(0, 0)
    cc_copy[1].wait_recv()
    z_step(1, 0)
    g_y[2, 0].wait_recv()
    g_y[2, 1].wait_recv()
    hg_other(2)
    x_direct(1)
    x_summed(1)
    x_direct(0)
    z_step(0, 1)
    z_step(1, 1)
    wg_add(2, 256, 768, True)
    wg_add(3, 256, 768, True)
    g_y[0, 0].wait_recv()
    g_y[0, 1].wait_recv()
    wg_add(2, 0, 256, False)
    cc_send(2)
    z_step(0, 2)
    wg_add(3, 0, 256, False)
    cc_send(3)
    z_step(1, 2)
    x_summed(0)
    cc_copy[2].wait_recv()
    z_step(2, 0)
    cc_copy[3].wait_recv()
    z_step(3, 0)
    hg_other(0)
    z_step(0, 3)
    z_step(1, 3)
    z_step(2, 1)
    z_step(3, 1)
    lo, hi = x_total(1)
    yos[:, left] = lo
    yos[:, right] = hi
    start(o_y)
    z_last(0)
    send_fin(0)
    z_last(1)
    send_fin(1)
    z_step(2, 2)
    z_step(3, 2)
    z_step(2, 3)
    z_step(3, 3)
    lo, hi = x_total(0)
    os[:, left] = lo
    os[:, right] = hi
    put_mine = local(os, out_ref.at[:, mine], 5)
    o_y.wait_recv()
    put_other = local(yor, out_ref.at[:, other], 6)
    z_last(2)
    send_fin(2)
    z_last(3)
    send_fin(3)

    def arrived(slot, n):
        pltpu.make_async_copy(yr.at[slot, n], yr.at[slot, n], yrsem.at[slot, n]).wait()

    for n in range(2):
        chunk = pl.ds(n * CW, CW)

        @pl.when(yh == yl)
        def _():
            arrived(1 - yh, n)
            gs[:, chunk] = fin[n].astype(F32) + yr[1 - yh, n].astype(F32)

        @pl.when(yh != yl)
        def _():
            arrived(0, n)
            arrived(1, n)
            gs[:, chunk] = yr[0, n].astype(F32) + yr[1, n].astype(F32)

    puts = [
        local(gs.at[:, pl.ds(0, CQ)], gq_ref, 7),
        local(gs.at[:, pl.ds(CQ, CK)], gk_ref, 8),
        local(gs.at[:, pl.ds(CQ + CK, CK)], gv_ref, 9),
    ]

    @pl.when(yh != yl)
    def _():
        last[0].wait_send()
        last[1].wait_send()

    last[2].wait_send()
    last[3].wait_send()
    for copy in sent:
        copy.wait_send()
    for put in [put_mine, put_other] + puts:
        put.wait()


def hand_over(*refs):
    sources, targets, through, (into, out) = refs[:4], refs[4:8], refs[8:12], refs[12:]
    loads = [pltpu.make_async_copy(sources[i], through[i], into.at[i]) for i in range(4)]
    stores = [pltpu.make_async_copy(through[i], targets[i], out.at[i]) for i in range(4)]
    for load in loads:
        load.start()
    for load, store in zip(loads, stores):
        load.wait()
        store.start()
    for store in stores:
        store.wait()


N_SEM = 96


def local_step(*args):
    scratch = [
        pltpu.VMEM((1024, H), BF16),
        pltpu.VMEM((T, H), BF16),
        pltpu.VMEM((1024, C), BF16),
        pltpu.VMEM((1024, C), BF16),
        pltpu.VMEM((H, C), BF16),
        pltpu.VMEM((H, C), BF16),
        pltpu.VMEM((C, H), BF16),
        pltpu.VMEM((512, C), BF16),
        pltpu.VMEM((1024, H), F32),
        pltpu.VMEM((4, H, CW), F32),
        pltpu.VMEM((4, 1024, CW), BF16),
        pltpu.VMEM((4, 1024, CW), BF16),
        pltpu.VMEM((2, 3, 2, T, HH), BF16),
        pltpu.VMEM((2, 3, 2, T, HH), BF16),
        pltpu.VMEM((4, 2, 448, CW), BF16),
        pltpu.VMEM((4, 2, 448, CW), BF16),
        pltpu.VMEM((4, T, CW), BF16),
        pltpu.VMEM((2, 2, T, CW), BF16),
        pltpu.VMEM((T, H), BF16),
        pltpu.VMEM((T, H), BF16),
        pltpu.VMEM((T, H), BF16),
        pltpu.VMEM((T, C), F32),
        pltpu.SemaphoreType.DMA((10,)),
        pltpu.SemaphoreType.DMA((N_SEM,)),
        pltpu.SemaphoreType.DMA((N_SEM,)),
        pltpu.SemaphoreType.DMA((4,)),
        pltpu.SemaphoreType.DMA((2, 2)),
    ]
    anywhere = pl.BlockSpec(memory_space=pl.ANY)
    shapes = [((T, D), BF16), ((T, CQ), F32), ((T, CK), F32), ((T, CK), F32)]
    out_shape = tuple(jax.ShapeDtypeStruct(*shape) for shape in shapes)
    results = pl.pallas_call(
        kernel,
        out_shape=out_shape,
        in_specs=[anywhere] * 7,
        out_specs=(anywhere,) * 4,
        scratch_shapes=scratch,
        compiler_params=pltpu.CompilerParams(
            collective_id=0, has_side_effects=True, vmem_limit_bytes=67043328
        ),
    )(*args)
    return pl.pallas_call(
        hand_over,
        out_shape=out_shape,
        in_specs=[anywhere] * 4,
        out_specs=(anywhere,) * 4,
        scratch_shapes=[pltpu.VMEM(*shape) for shape in shapes]
        + [pltpu.SemaphoreType.DMA((4,)), pltpu.SemaphoreType.DMA((4,))],
        cost_estimate=pl.CostEstimate(flops=0, bytes_accessed=3 << 20, transcendentals=0),
    )(*results)


def solution(mesh):
    both = P(("dp", "tp"), None)
    split = P("dp", "tp")
    return jax.shard_map(
        local_step,
        mesh=mesh,
        in_specs=(both, split, split, split, P(None, "tp"), P(None, "tp"), P(None, "tp")),
        out_specs=(both, split, split, split),
        check_vma=False,
    )
```

```python
import jax
import jax.numpy as jnp
from jax import lax
from jax.experimental import pallas as pl
from jax.experimental.pallas import tpu as pltpu
from jax.sharding import PartitionSpec as P

MESH = pl.DeviceIdType.MESH
BF16 = jnp.bfloat16
F32 = jnp.float32
T = 128
D = 4096
H = 2048
HH = 1024
CQ = 512
CK = 128
C = 768
CW = 384


def nt(left, right):
    return lax.dot_general(left, right, (((1,), (1,)), ((), ())), preferred_element_type=F32)


def tn(left, right):
    return lax.dot_general(left, right, (((0,), (0,)), ((), ())), preferred_element_type=F32)


def kernel(
    hidden_ref,
    q_ref,
    k_ref,
    v_ref,
    wq_ref,
    wk_ref,
    wv_ref,
    out_ref,
    gq_ref,
    gk_ref,
    gv_ref,
    hid,
    hsend,
    gown,
    goth,
    wh,
    woth,
    wt,
    wsend,
    hg,
    wg,
    ccs,
    ccr,
    xs,
    xr,
    zs,
    zr,
    fin,
    yr,
    yos,
    yor,
    os,
    gs,
    lsem,
    ssem,
    rsem,
    yssem,
    yrsem,
):
    dp = lax.axis_index("dp")
    tp = lax.axis_index("tp")
    c = lax.rem(dp, 2)
    z = lax.rem(dp // 2, 8)
    yh = dp // 16
    yl = lax.rem(tp, 2)
    x = tp // 2
    e = lax.rem(z, 2)

    def dev(xx=None, yhh=None, yll=None, zz=None, cc=None):
        xx = x if xx is None else xx
        yhh = yh if yhh is None else yhh
        yll = yl if yll is None else yll
        zz = z if zz is None else zz
        cc = c if cc is None else cc
        return (yhh * 16 + zz * 2 + cc, xx * 2 + yll)

    XP = dev(xx=lax.rem(x + 1, 4))
    XM = dev(xx=lax.rem(x + 3, 4))
    YI = dev(yll=1 - yl)
    YO = dev(yhh=1 - yh, yll=1 - yl)
    Y2 = dev(yhh=1 - yh)
    ZP = dev(zz=lax.rem(z + 1, 8))
    ZM = dev(zz=lax.rem(z + 7, 8))
    ZX = dev(zz=z + 1 - 2 * e)
    CC = dev(cc=1 - c)

    counter = [0]
    sent = []

    def remote(src, dst, target, send=None, recv=None):
        if send is None:
            i = counter[0]
            counter[0] += 1
            send, recv = ssem.at[i], rsem.at[i]
        copy = pltpu.make_async_remote_copy(
            src_ref=src, dst_ref=dst, send_sem=send, recv_sem=recv, device_id=target, device_id_type=MESH
        )
        return copy

    def start(copy):
        copy.start()
        if not any(copy is one for one in sent):
            sent.append(copy)

    def local(src, dst, i):
        copy = pltpu.make_async_copy(src, dst, lsem.at[i])
        copy.start()
        return copy

    mine = pl.ds(pl.multiple_of(yl * H, H), H)
    other = pl.ds(pl.multiple_of((1 - yl) * H, H), H)
    for h in range(2):
        for zz in range(8):
            first = pl.multiple_of(yl * H + (2 * zz + h) * T, T)
            local(hidden_ref.at[:, pl.ds(first, T)], hid.at[h, zz, pl.ds(0, T)], 0 if h == 0 else 10)
    for h in range(2):
        for zz in range(8):
            first = pl.multiple_of((1 - yl) * H + (2 * zz + h) * T, T)
            local(hidden_ref.at[:, pl.ds(first, T)], hsend.at[h, zz], 1)
    wrow = c * 1024 + e * 512
    wrows = pl.ds(pl.multiple_of((1 - yl) * H + wrow, 512), 512)
    local(wq_ref.at[wrows], wsend.at[:, pl.ds(0, CQ)], 2)
    local(wk_ref.at[wrows], wsend.at[:, pl.ds(CQ, CK)], 2)
    local(wv_ref.at[wrows], wsend.at[:, pl.ds(CQ + CK, CK)], 2)
    for r, off in enumerate((0, 1, 3, 2)):
        for s in range(2):
            block = lax.rem(x + off, 4) * 2 + (yl if s == 0 else 1 - yl)
            src = pl.ds(pl.multiple_of(block * T, T), T)
            dst = pl.ds(r * 256 + s * T, T)
            local(q_ref.at[src], gown.at[dst, pl.ds(0, CQ)], 3)
            local(k_ref.at[src], gown.at[dst, pl.ds(CQ, CK)], 3)
            local(v_ref.at[src], gown.at[dst, pl.ds(CQ + CK, CK)], 3)
    local(wq_ref.at[mine], wh.at[:, pl.ds(0, CQ)], 4)
    local(wk_ref.at[mine], wh.at[:, pl.ds(CQ, CK)], 4)
    local(wv_ref.at[mine], wh.at[:, pl.ds(CQ + CK, CK)], 4)

    def wait_local(buffer, i):
        pltpu.make_async_copy(buffer, buffer, lsem.at[i]).wait()

    barrier = pltpu.get_barrier_semaphore()
    for target in (XP, XM, YI, YO, Y2, ZP, ZM, CC):
        pl.semaphore_signal(barrier, inc=1, device_id=target, device_id_type=MESH)
    pl.semaphore_wait(barrier, 8)

    def rows(r, s, half=None):
        first = r * 256 + s * T
        return pl.ds(first, T) if half is None else pl.ds(first + half * 64, 64)

    def piece(h, r, s, i):
        return hid.at[h, :, rows(r, s, i)]

    both = range(2)
    a_p = [[remote(piece(h, 0, 0, i), piece(h, 2, 0, i), XP) for i in both] for h in both]
    a_m = [[remote(piece(h, 0, 0, i), piece(h, 1, 0, i), XM) for i in both] for h in both]
    b_y = [remote(hsend.at[h], hid.at[h, :, rows(0, 1)], YI) for h in both]
    b_p = [[remote(piece(h, 0, 1, i), piece(h, 2, 1, i), XP) for i in both] for h in both]
    b_m = [[remote(piece(h, 0, 1, i), piece(h, 1, 1, i), XM) for i in both] for h in both]
    f_p = [[remote(piece(h, 2, s, 0), piece(h, 3, s, 0), XP) for s in both] for h in both]
    f_m = [[remote(piece(h, 1, s, 1), piece(h, 3, s, 1), XM) for s in both] for h in both]
    g_y = {
        (r, s): remote(gown.at[rows(r, s)], goth.at[rows(r, 1 - s)], YI) for r in (3, 1, 2, 0) for s in range(2)
    }

    def wpiece(cc, ee, k):
        return pl.ds(pl.multiple_of(cc * 1024 + ee * 512 + k * 256, 256), 256)

    w_y = [remote(wsend.at[pl.ds(256 * k, 256)], woth.at[wpiece(c, e, k)], YO) for k in range(2)]
    w_z = [remote(woth.at[wpiece(c, e, k)], woth.at[wpiece(c, e, k)], ZX) for k in range(2)]
    w_c = [remote(woth.at[wpiece(c, e, k)], woth.at[wpiece(c, e, k)], CC) for k in range(2)]
    w_d = [remote(woth.at[wpiece(c, 1 - e, k)], woth.at[wpiece(c, 1 - e, k)], CC) for k in range(2)]
    xc = {
        (d, b, s): remote(xs.at[d, b, s], xr.at[d, b, s], XP if d == 0 else XM)
        for d in range(2)
        for b in range(3)
        for s in range(2)
    }
    o_y = remote(yos, yor, YI)
    cc_copy = [remote(ccs.at[n], ccr.at[n], CC) for n in range(4)]
    steps = (pl.ds(0, 64), pl.ds(64, 128), pl.ds(192, 128), pl.ds(320, 128))
    zc = {
        (n, d, i): remote(zs.at[n, d, steps[i]], zr.at[n, d, steps[i]], ZP if d == 0 else ZM)
        for n in range(4)
        for d in range(2)
        for i in range(4)
    }

    wait_local(hid.at[0, :, pl.ds(0, T)], 0)
    for i in range(2):
        start(a_p[0][i])
        start(a_m[0][1 - i])
    wait_local(hsend, 1)
    start(b_y[0])
    wait_local(wsend, 2)
    for k in range(2):
        start(w_y[k])
    wait_local(gown, 3)
    for r in (3, 1, 2, 0):
        for s in (0, 1):
            start(g_y[r, s])
        if r == 3:
            start(b_y[1])
    wait_local(hid.at[1, :, pl.ds(0, T)], 10)
    wait_local(wh.at[:, pl.ds(0, C)], 4)

    def hg_own():
        def step(n, carry):
            cols = pl.ds(pl.multiple_of(n * 256, 256), 256)
            w = wh[cols, :C]
            for m in range(2):
                hg[pl.ds(m * 512, 512), cols] = nt(gown[pl.ds(m * 512, 512), :], w)
            return carry

        lax.fori_loop(0, 8, step, 0)

    def turn(cc, ee, k):
        piece = wpiece(cc, ee, k)
        wt[:, piece] = woth[piece, :].T

    def hg_other(r):
        def step(n, carry):
            cols = pl.ds(pl.multiple_of(n * 512, 512), 512)
            block = pl.ds(r * 256, 256)
            hg[block, cols] += jnp.dot(goth[block, :], wt[:, cols], preferred_element_type=F32)
            return carry

        lax.fori_loop(0, 4, step, 0)

    def flip(h, r):
        def step(zz, carry):
            dst = pl.ds(pl.multiple_of(h * 1024 + zz * T, T), T)
            block = pl.ds(r * 256, 256)
            wh[dst, block] = hid[h, zz, block, :].T
            return carry

        lax.fori_loop(0, 8, step, 0)

    def wg_add(pair, h, first, depth, fresh):
        g = goth if pair else gown
        toks = pl.ds(first, depth)

        def step(m, carry):
            block = pl.ds(pl.multiple_of(h * 1024 + m * 512, 512), 512)
            part = jnp.dot(wh[block, toks], g[toks, :], preferred_element_type=F32)
            for i in range(2):
                cut = part[:, i * CW : (i + 1) * CW]
                wg[2 * pair + i, block, :] = cut if fresh else wg[2 * pair + i, block, :] + cut
            return carry

        lax.fori_loop(0, 2, step, 0)

    def cc_send(n, h):
        @pl.when(c != h)
        def _():
            for m in range(4):
                ccs[n, pl.ds(m * 256, 256), :] = wg[n, pl.ds(h * 1024 + m * 256, 256), :].astype(BF16)
            start(cc_copy[n])

    def pair_sum(n, zz, first=0, size=T):
        src = pl.ds(pl.multiple_of(c * 1024 + zz * T + first, size), size)
        dst = pl.ds(pl.multiple_of(zz * T + first, size), size)
        return wg[n, src, :] + ccr[n, dst, :].astype(F32)

    def z_own(i):
        for n in range(2):
            z_any(n, i)

    def z_other(i):
        for n in range(2, 4):
            z_any(n, i)

    def z_any(n, i):
        if i == 0:
            cc_copy[n].wait_recv()
        if i < 4:
            z_step(n, i)
        else:
            z_last(n)
            send_fin(n)

    def on_core(h, work, *args):
        @pl.when(c == h)
        def _():
            work(*args)

    def z_step(n, i):
        if i == 0:
            far = lax.rem(z + 4, 8)
            zs[n, 0, steps[0], :] = pair_sum(n, far, 0, 64).astype(BF16)
            zs[n, 1, steps[0], :] = pair_sum(n, far, 64, 64).astype(BF16)
        else:
            for d in range(2):
                zz = lax.rem(z + 4 - i, 8) if d == 0 else lax.rem(z + 4 + i, 8)
                zc[n, d, i - 1].wait_recv()
                if i == 1:
                    for half in range(2):
                        part = pair_sum(n, zz, half * 64, 64)
                        if half == d:
                            part = part + zr[n, d, steps[0], :].astype(F32)
                        zs[n, d, pl.ds(64 + half * 64, 64), :] = part.astype(BF16)
                else:
                    part = pair_sum(n, zz) + zr[n, d, steps[i - 1], :].astype(F32)
                    zs[n, d, steps[i], :] = part.astype(BF16)
                start(zc[n, d, i])
        if i == 0:
            for d in range(2):
                start(zc[n, d, 0])

    def z_last(n):
        for d in range(2):
            zc[n, d, 3].wait_recv()
        total = pair_sum(n, z) + zr[n, 0, steps[3], :].astype(F32) + zr[n, 1, steps[3], :].astype(F32)
        fin[n] = total.astype(BF16)

    left, right = pl.ds(0, HH), pl.ds(HH, HH)

    def x_far():
        for s in (1, 0):
            block = pl.ds(3 * 256 + s * T, T)
            xs[0, 0, s] = hg[block, left].astype(BF16)
            start(xc[0, 0, s])
            xs[1, 0, s] = hg[block, right].astype(BF16)
            start(xc[1, 0, s])

    def x_direct(s):
        xs[0, 1, s] = hg[pl.ds(1 * 256 + s * T, T), right].astype(BF16)
        start(xc[0, 1, s])
        xs[1, 1, s] = hg[pl.ds(2 * 256 + s * T, T), left].astype(BF16)
        start(xc[1, 1, s])

    def x_summed(s):
        xc[0, 0, s].wait_recv()
        xs[0, 2, s] = (hg[pl.ds(1 * 256 + s * T, T), left] + xr[0, 0, s].astype(F32)).astype(BF16)
        start(xc[0, 2, s])
        xc[1, 0, s].wait_recv()
        xs[1, 2, s] = (hg[pl.ds(2 * 256 + s * T, T), right] + xr[1, 0, s].astype(F32)).astype(BF16)
        start(xc[1, 2, s])

    def x_total(s):
        for d in range(2):
            xc[d, 1, s].wait_recv()
            xc[d, 2, s].wait_recv()
        block = pl.ds(s * T, T)
        lo = hg[block, left] + xr[0, 2, s].astype(F32) + xr[1, 1, s].astype(F32)
        hi = hg[block, right] + xr[0, 1, s].astype(F32) + xr[1, 2, s].astype(F32)
        return lo.astype(BF16), hi.astype(BF16)

    def send_fin(n):
        if n < 2:

            @pl.when(yh != yl)
            def _():
                last[n].start()
        else:
            last[n].start()

    last = [
        remote(
            fin.at[n],
            yr.at[yh, n % 2],
            dev(yhh=yl) if n < 2 else dev(yhh=yl, yll=1 - yl),
            yssem.at[n],
            yrsem.at[yh, n % 2],
        )
        for n in range(4)
    ]

    def hid_in(h, r):
        if r == 3:
            for s in range(2):
                f_p[h][s].wait_recv()
                f_m[h][s].wait_recv()
        else:
            copies = (a_p[h], b_p[h]) if r == 2 else (a_m[h], b_m[h])
            i = 1 if r == 2 else 0
            for copy in copies:
                copy[i].wait_recv()

    def forward(h, s):
        src_p, src_m = (b_p, b_m) if s else (a_p, a_m)
        src_p[h][0].wait_recv()
        start(f_p[h][s])
        src_m[h][1].wait_recv()
        start(f_m[h][s])

    def send_b(h):
        b_y[h].wait_recv()
        for i in range(2):
            start(b_p[h][i])
            start(b_m[h][1 - i])

    def g_in(r):
        g_y[r, 0].wait_recv()
        g_y[r, 1].wait_recv()

    hg_own()
    forward(0, 0)
    send_b(0)
    flip(0, 0)
    wg_add(0, 0, 0, 256, True)
    w_y[0].wait_recv()
    start(w_z[0])
    start(w_c[0])
    forward(0, 1)
    for i in range(2):
        start(a_p[1][i])
        start(a_m[1][1 - i])
    turn(c, e, 0)
    hid_in(0, 1)
    hid_in(0, 2)
    flip(0, 1)
    flip(0, 2)
    wg_add(0, 0, 256, 512, False)
    w_y[1].wait_recv()
    start(w_z[1])
    start(w_c[1])
    w_c[0].wait_recv()
    turn(1 - c, e, 0)
    hid_in(0, 3)
    flip(0, 3)
    wg_add(0, 0, 768, 256, False)
    cc_send(0, 0)
    cc_send(1, 0)
    w_z[0].wait_recv()
    start(w_d[0])
    forward(1, 0)
    send_b(1)
    on_core(0, z_own, 0)
    turn(c, e, 1)
    turn(c, 1 - e, 0)
    flip(1, 0)
    wg_add(0, 1, 0, 256, True)
    w_c[1].wait_recv()
    turn(1 - c, e, 1)
    w_d[0].wait_recv()
    turn(1 - c, 1 - e, 0)
    w_z[1].wait_recv()
    start(w_d[1])
    turn(c, 1 - e, 1)
    g_in(3)
    w_d[1].wait_recv()
    turn(1 - c, 1 - e, 1)
    on_core(0, z_own, 1)
    hg_other(3)
    forward(1, 1)
    x_far()
    hid_in(1, 1)
    hid_in(1, 2)
    on_core(0, z_own, 2)
    flip(1, 1)
    flip(1, 2)
    wg_add(0, 1, 256, 512, False)
    hid_in(1, 3)
    flip(1, 3)
    wg_add(0, 1, 768, 256, False)
    cc_send(0, 1)
    cc_send(1, 1)
    g_in(1)
    hg_other(1)
    g_in(2)
    hg_other(2)
    x_direct(1)
    on_core(1, z_own, 0)
    wg_add(1, 0, 256, 768, True)
    on_core(0, z_own, 3)
    x_summed(1)
    x_direct(0)
    on_core(1, z_own, 1)
    wg_add(1, 1, 256, 768, True)
    g_in(0)
    for h in range(2):
        wg_add(1, h, 0, 256, False)
        cc_send(2, h)
        cc_send(3, h)
    on_core(0, z_own, 4)
    on_core(1, z_own, 2)
    x_summed(0)
    z_other(0)
    hg_other(0)
    on_core(1, z_own, 3)
    z_other(1)
    on_core(1, z_own, 4)
    lo, hi = x_total(1)
    yos[:, left] = lo
    yos[:, right] = hi
    start(o_y)
    z_other(2)
    z_other(3)
    z_any(2, 4)
    lo, hi = x_total(0)
    os[:, left] = lo
    os[:, right] = hi
    put_mine = local(os, out_ref.at[:, mine], 5)
    z_any(3, 4)
    o_y.wait_recv()
    put_other = local(yor, out_ref.at[:, other], 6)

    def arrived(slot, n):
        pltpu.make_async_copy(yr.at[slot, n], yr.at[slot, n], yrsem.at[slot, n]).wait()

    for n in range(2):
        chunk = pl.ds(n * CW, CW)

        @pl.when(yh == yl)
        def _():
            arrived(1 - yh, n)
            gs[:, chunk] = fin[n].astype(F32) + yr[1 - yh, n].astype(F32)

        @pl.when(yh != yl)
        def _():
            arrived(0, n)
            arrived(1, n)
            gs[:, chunk] = yr[0, n].astype(F32) + yr[1, n].astype(F32)

    puts = [
        local(gs.at[:, pl.ds(0, CQ)], gq_ref, 7),
        local(gs.at[:, pl.ds(CQ, CK)], gk_ref, 8),
        local(gs.at[:, pl.ds(CQ + CK, CK)], gv_ref, 9),
    ]

    @pl.when(yh != yl)
    def _():
        last[0].wait_send()
        last[1].wait_send()

    last[2].wait_send()
    last[3].wait_send()
    for copy in sent:
        copy.wait_send()
    for put in [put_mine, put_other] + puts:
        put.wait()


def hand_over(*refs):
    sources, targets, through, (into, out) = refs[:4], refs[4:8], refs[8:12], refs[12:]
    loads = [pltpu.make_async_copy(sources[i], through[i], into.at[i]) for i in range(4)]
    stores = [pltpu.make_async_copy(through[i], targets[i], out.at[i]) for i in range(4)]
    for load in loads:
        load.start()
    for load, store in zip(loads, stores):
        load.wait()
        store.start()
    for store in stores:
        store.wait()


N_SEM = 96


def local_step(*args):
    scratch = [
        pltpu.VMEM((2, 8, 1024, T), BF16),
        pltpu.VMEM((2, 8, T, T), BF16),
        pltpu.VMEM((1024, C), BF16),
        pltpu.VMEM((1024, C), BF16),
        pltpu.VMEM((H, 1024), BF16),
        pltpu.VMEM((H, C), BF16),
        pltpu.VMEM((C, H), BF16),
        pltpu.VMEM((512, C), BF16),
        pltpu.VMEM((1024, H), F32),
        pltpu.VMEM((4, H, CW), F32),
        pltpu.VMEM((4, 1024, CW), BF16),
        pltpu.VMEM((4, 1024, CW), BF16),
        pltpu.VMEM((2, 3, 2, T, HH), BF16),
        pltpu.VMEM((2, 3, 2, T, HH), BF16),
        pltpu.VMEM((4, 2, 448, CW), BF16),
        pltpu.VMEM((4, 2, 448, CW), BF16),
        pltpu.VMEM((4, T, CW), BF16),
        pltpu.VMEM((2, 2, T, CW), BF16),
        pltpu.VMEM((T, H), BF16),
        pltpu.VMEM((T, H), BF16),
        pltpu.VMEM((T, H), BF16),
        pltpu.VMEM((T, C), F32),
        pltpu.SemaphoreType.DMA((11,)),
        pltpu.SemaphoreType.DMA((N_SEM,)),
        pltpu.SemaphoreType.DMA((N_SEM,)),
        pltpu.SemaphoreType.DMA((4,)),
        pltpu.SemaphoreType.DMA((2, 2)),
    ]
    anywhere = pl.BlockSpec(memory_space=pl.ANY)
    shapes = [((T, D), BF16), ((T, CQ), F32), ((T, CK), F32), ((T, CK), F32)]
    out_shape = tuple(jax.ShapeDtypeStruct(*shape) for shape in shapes)
    results = pl.pallas_call(
        kernel,
        out_shape=out_shape,
        in_specs=[anywhere] * 7,
        out_specs=(anywhere,) * 4,
        scratch_shapes=scratch,
        compiler_params=pltpu.CompilerParams(
            collective_id=0, has_side_effects=True, vmem_limit_bytes=67043328
        ),
    )(*args)
    return pl.pallas_call(
        hand_over,
        out_shape=out_shape,
        in_specs=[anywhere] * 4,
        out_specs=(anywhere,) * 4,
        scratch_shapes=[pltpu.VMEM(*shape) for shape in shapes]
        + [pltpu.SemaphoreType.DMA((4,)), pltpu.SemaphoreType.DMA((4,))],
        cost_estimate=pl.CostEstimate(flops=0, bytes_accessed=3 << 20, transcendentals=0),
    )(*results)


def solution(mesh):
    both = P(("dp", "tp"), None)
    split = P("dp", "tp")
    return jax.shard_map(
        local_step,
        mesh=mesh,
        in_specs=(both, split, split, split, P(None, "tp"), P(None, "tp"), P(None, "tp")),
        out_specs=(both, split, split, split),
        check_vma=False,
    )
```

```python
import jax
import jax.numpy as jnp
from jax import lax
from jax.experimental import pallas as pl
from jax.experimental.pallas import tpu as pltpu
from jax.sharding import PartitionSpec as P

MESH = pl.DeviceIdType.MESH
BF16 = jnp.bfloat16
F32 = jnp.float32
T = 128
D = 4096
H = 2048
HH = 1024
CQ = 512
CK = 128
C = 768
CHUNKS = ((0, 0, 384), (0, 384, 384), (1, 0, 256), (1, 256, 256), (1, 512, 256))
OWN = (0, 1)
PAIR = (2, 3, 4)


def nt(left, right):
    return lax.dot_general(left, right, (((1,), (1,)), ((), ())), preferred_element_type=F32)


def tn(left, right):
    return lax.dot_general(left, right, (((0,), (0,)), ((), ())), preferred_element_type=F32)


def kernel(
    hidden_ref,
    q_ref,
    k_ref,
    v_ref,
    wq_ref,
    wk_ref,
    wv_ref,
    out_ref,
    yr,
    hid,
    hsend,
    gown,
    goth,
    wh,
    woth,
    wt,
    wsend,
    hg,
    wg,
    ccs,
    ccr,
    xs,
    xr,
    zs,
    zr,
    fin,
    yos,
    os,
    lsem,
    ssem,
    rsem,
    yssem,
    yrsem,
):
    dp = lax.axis_index("dp")
    tp = lax.axis_index("tp")
    c = lax.rem(dp, 2)
    z = lax.rem(dp // 2, 8)
    yh = dp // 16
    yl = lax.rem(tp, 2)
    x = tp // 2
    e = lax.rem(z, 2)

    def dev(xx=None, yhh=None, yll=None, zz=None, cc=None):
        xx = x if xx is None else xx
        yhh = yh if yhh is None else yhh
        yll = yl if yll is None else yll
        zz = z if zz is None else zz
        cc = c if cc is None else cc
        return (yhh * 16 + zz * 2 + cc, xx * 2 + yll)

    XP = dev(xx=lax.rem(x + 1, 4))
    XM = dev(xx=lax.rem(x + 3, 4))
    YI = dev(yll=1 - yl)
    YO = dev(yhh=1 - yh, yll=1 - yl)
    Y2 = dev(yhh=1 - yh)
    ZP = dev(zz=lax.rem(z + 1, 8))
    ZM = dev(zz=lax.rem(z + 7, 8))
    ZX = dev(zz=z + 1 - 2 * e)
    CC = dev(cc=1 - c)

    counter = [0]
    sent = []

    def remote(src, dst, target, send=None, recv=None):
        if send is None:
            i = counter[0]
            counter[0] += 1
            send, recv = ssem.at[i], rsem.at[i]
        copy = pltpu.make_async_remote_copy(
            src_ref=src, dst_ref=dst, send_sem=send, recv_sem=recv, device_id=target, device_id_type=MESH
        )
        return copy

    def start(copy):
        copy.start()
        if not any(copy is one for one in sent):
            sent.append(copy)

    def local(src, dst, i):
        copy = pltpu.make_async_copy(src, dst, lsem.at[i])
        copy.start()
        return copy

    mine = pl.ds(pl.multiple_of(yl * H, H), H)
    other = pl.ds(pl.multiple_of((1 - yl) * H, H), H)
    for h in range(2):
        for zz in range(8):
            first = pl.multiple_of(yl * H + (2 * zz + h) * T, T)
            local(hidden_ref.at[:, pl.ds(first, T)], hid.at[h, zz, pl.ds(0, T)], 0 if h == 0 else 10)
    for h in range(2):
        for zz in range(8):
            first = pl.multiple_of((1 - yl) * H + (2 * zz + h) * T, T)
            local(hidden_ref.at[:, pl.ds(first, T)], hsend.at[h, zz], 1)
    wrow = c * 1024 + e * 512
    wrows = pl.ds(pl.multiple_of((1 - yl) * H + wrow, 512), 512)
    local(wq_ref.at[wrows], wsend.at[:, pl.ds(0, CQ)], 2)
    local(wk_ref.at[wrows], wsend.at[:, pl.ds(CQ, CK)], 2)
    local(wv_ref.at[wrows], wsend.at[:, pl.ds(CQ + CK, CK)], 2)
    for r, off in enumerate((0, 1, 3, 2)):
        for s in range(2):
            block = lax.rem(x + off, 4) * 2 + (yl if s == 0 else 1 - yl)
            src = pl.ds(pl.multiple_of(block * T, T), T)
            dst = pl.ds(r * 256 + s * T, T)
            local(q_ref.at[src], gown.at[dst, pl.ds(0, CQ)], 3)
            local(k_ref.at[src], gown.at[dst, pl.ds(CQ, CK)], 3)
            local(v_ref.at[src], gown.at[dst, pl.ds(CQ + CK, CK)], 3)
    local(wq_ref.at[mine], wh.at[:, pl.ds(0, CQ)], 4)
    local(wk_ref.at[mine], wh.at[:, pl.ds(CQ, CK)], 4)
    local(wv_ref.at[mine], wh.at[:, pl.ds(CQ + CK, CK)], 4)

    def wait_local(buffer, i):
        pltpu.make_async_copy(buffer, buffer, lsem.at[i]).wait()

    barrier = pltpu.get_barrier_semaphore()
    for target in (XP, XM, YI, YO, Y2, ZP, ZM, CC):
        pl.semaphore_signal(barrier, inc=1, device_id=target, device_id_type=MESH)
    pl.semaphore_wait(barrier, 8)

    def rows(r, s, half=None):
        first = r * 256 + s * T
        return pl.ds(first, T) if half is None else pl.ds(first + half * 64, 64)

    def piece(h, r, s, i):
        return hid.at[h, :, rows(r, s, i)]

    both = range(2)
    a_p = [[remote(piece(h, 0, 0, i), piece(h, 2, 0, i), XP) for i in both] for h in both]
    a_m = [[remote(piece(h, 0, 0, i), piece(h, 1, 0, i), XM) for i in both] for h in both]
    b_y = [remote(hsend.at[h], hid.at[h, :, rows(0, 1)], YI) for h in both]
    b_p = [[remote(piece(h, 0, 1, i), piece(h, 2, 1, i), XP) for i in both] for h in both]
    b_m = [[remote(piece(h, 0, 1, i), piece(h, 1, 1, i), XM) for i in both] for h in both]
    f_p = [[remote(piece(h, 2, s, 0), piece(h, 3, s, 0), XP) for s in both] for h in both]
    f_m = [[remote(piece(h, 1, s, 1), piece(h, 3, s, 1), XM) for s in both] for h in both]
    g_y = {
        (r, s): remote(gown.at[rows(r, s)], goth.at[rows(r, 1 - s)], YI) for r in (3, 1, 2, 0) for s in range(2)
    }

    def wpiece(cc, ee, k):
        return pl.ds(pl.multiple_of(cc * 1024 + ee * 512 + k * 128, 128), 128)

    w_y = [remote(wsend.at[pl.ds(128 * k, 128)], woth.at[wpiece(c, e, k)], YO) for k in range(4)]
    w_z = [remote(woth.at[wpiece(c, e, k)], woth.at[wpiece(c, e, k)], ZX) for k in range(4)]
    w_c = [remote(woth.at[wpiece(c, e, k)], woth.at[wpiece(c, e, k)], CC) for k in range(4)]
    w_d = [remote(woth.at[wpiece(c, 1 - e, k)], woth.at[wpiece(c, 1 - e, k)], CC) for k in range(4)]
    xc = {
        (d, b, s): remote(xs.at[d, b, s], xr.at[d, b, s], XP if d == 0 else XM)
        for d in range(2)
        for b in range(3)
        for s in range(2)
    }
    o_y = remote(yos, out_ref.at[:, mine], YI)
    cc_copy = []
    for n, (p, first, width) in enumerate(CHUNKS):
        cols = pl.ds(first, width)
        cc_copy.append(remote(ccs.at[p, :, cols], ccr.at[p, :, cols], CC))
    steps = (pl.ds(0, 64), pl.ds(64, 128), pl.ds(192, 128), pl.ds(320, 128))
    zc = {}
    for n, (p, first, width) in enumerate(CHUNKS):
        cols = pl.ds(first, width)
        for d in range(2):
            for i in range(4):
                part = (p, d, steps[i], cols)
                zc[n, d, i] = remote(zs.at[part], zr.at[part], ZP if d == 0 else ZM)

    wait_local(hid.at[0, :, pl.ds(0, T)], 0)
    for i in range(2):
        start(a_p[0][i])
        start(a_m[0][1 - i])
    wait_local(hsend, 1)
    start(b_y[0])
    wait_local(wsend, 2)
    for k in range(4):
        start(w_y[k])
    wait_local(gown, 3)
    for r in (3, 1, 2, 0):
        for s in (0, 1):
            start(g_y[r, s])
        if r == 3:
            start(b_y[1])
    wait_local(hid.at[1, :, pl.ds(0, T)], 10)
    wait_local(wh.at[:, pl.ds(0, C)], 4)

    def hg_own():
        def step(n, carry):
            cols = pl.ds(pl.multiple_of(n * 256, 256), 256)
            w = wh[cols, :C]
            for m in range(2):
                hg[pl.ds(m * 512, 512), cols] = nt(gown[pl.ds(m * 512, 512), :], w)
            return carry

        lax.fori_loop(0, 8, step, 0)

    def turn(cc, ee, k):
        piece = wpiece(cc, ee, k)
        wt[:, piece] = woth[piece, :].T

    def hg_other(r, s=None):
        block = pl.ds(r * 256, 256) if s is None else pl.ds(r * 256 + s * T, T)

        def step(n, carry):
            cols = pl.ds(pl.multiple_of(n * 512, 512), 512)
            hg[block, cols] += jnp.dot(goth[block, :], wt[:, cols], preferred_element_type=F32)
            return carry

        lax.fori_loop(0, 4, step, 0)

    def flip(h, r):
        def step(zz, carry):
            dst = pl.ds(pl.multiple_of(h * 1024 + zz * T, T), T)
            block = pl.ds(r * 256, 256)
            wh[dst, block] = hid[h, zz, block, :].T
            return carry

        lax.fori_loop(0, 8, step, 0)

    def wg_add(pair, h, first, depth, fresh):
        g = goth if pair else gown
        toks = pl.ds(first, depth)

        def step(m, carry):
            block = pl.ds(pl.multiple_of(h * 1024 + m * 512, 512), 512)
            part = jnp.dot(wh[block, toks], g[toks, :], preferred_element_type=F32)
            wg[pair, block, :] = part if fresh else wg[pair, block, :] + part
            return carry

        lax.fori_loop(0, 2, step, 0)

    def cc_send(chunks, h):
        @pl.when(c != h)
        def _():
            for n in chunks:
                p, first, width = CHUNKS[n]
                cols = pl.ds(first, width)
                for m in range(4):
                    src = pl.ds(h * 1024 + m * 256, 256)
                    ccs[p, pl.ds(m * 256, 256), cols] = wg[p, src, cols].astype(BF16)
                start(cc_copy[n])

    def pair_sum(n, zz, start_row=0, size=T):
        p, first, width = CHUNKS[n]
        cols = pl.ds(first, width)
        src = pl.ds(pl.multiple_of(c * 1024 + zz * T + start_row, size), size)
        dst = pl.ds(pl.multiple_of(zz * T + start_row, size), size)
        return wg[p, src, cols] + ccr[p, dst, cols].astype(F32)

    def z_own(i):
        for n in OWN:
            z_any(n, i)

    def z_other(i):
        for n in PAIR:
            z_any(n, i)

    def z_any(n, i):
        if i == 0:
            cc_copy[n].wait_recv()
        if i < 4:
            z_step(n, i)
        else:
            z_last(n)
            send_fin(n)

    def reducer(h, work, *args):
        @pl.when(c == h)
        def _():
            work(*args)

    def z_step(n, i):
        p, first, width = CHUNKS[n]
        cols = pl.ds(first, width)
        if i == 0:
            far = lax.rem(z + 4, 8)
            for d in range(2):
                zs[p, d, steps[0], cols] = pair_sum(n, far, d * 64, 64).astype(BF16)
                start(zc[n, d, 0])
        for d in range(2) if i else ():
            zz = lax.rem(z + 4 - i, 8) if d == 0 else lax.rem(z + 4 + i, 8)
            zc[n, d, i - 1].wait_recv()
            came = zr[p, d, steps[i - 1], cols].astype(F32)
            if i == 1:
                for half in range(2):
                    part = pair_sum(n, zz, half * 64, 64)
                    if half == d:
                        part = part + came
                    zs[p, d, pl.ds(64 + half * 64, 64), cols] = part.astype(BF16)
            else:
                zs[p, d, steps[i], cols] = (pair_sum(n, zz) + came).astype(BF16)
            start(zc[n, d, i])

    def z_last(n):
        p, first, width = CHUNKS[n]
        cols = pl.ds(first, width)
        for d in range(2):
            zc[n, d, 3].wait_recv()
        came = zr[p, 0, steps[3], cols].astype(F32) + zr[p, 1, steps[3], cols].astype(F32)
        fin[p, :, cols] = (pair_sum(n, z) + came).astype(BF16)

    left, right = pl.ds(0, HH), pl.ds(HH, HH)

    def x_far(s):
        block = pl.ds(3 * 256 + s * T, T)
        xs[0, 0, s] = hg[block, left].astype(BF16)
        start(xc[0, 0, s])
        xs[1, 0, s] = hg[block, right].astype(BF16)
        start(xc[1, 0, s])

    def x_direct(s):
        xs[0, 1, s] = hg[pl.ds(1 * 256 + s * T, T), right].astype(BF16)
        start(xc[0, 1, s])
        xs[1, 1, s] = hg[pl.ds(2 * 256 + s * T, T), left].astype(BF16)
        start(xc[1, 1, s])

    def x_summed(s):
        xc[0, 0, s].wait_recv()
        xs[0, 2, s] = (hg[pl.ds(1 * 256 + s * T, T), left] + xr[0, 0, s].astype(F32)).astype(BF16)
        start(xc[0, 2, s])
        xc[1, 0, s].wait_recv()
        xs[1, 2, s] = (hg[pl.ds(2 * 256 + s * T, T), right] + xr[1, 0, s].astype(F32)).astype(BF16)
        start(xc[1, 2, s])

    def x_total(s):
        for d in range(2):
            xc[d, 1, s].wait_recv()
            xc[d, 2, s].wait_recv()
        block = pl.ds(s * T, T)
        lo = hg[block, left] + xr[0, 2, s].astype(F32) + xr[1, 1, s].astype(F32)
        hi = hg[block, right] + xr[0, 1, s].astype(F32) + xr[1, 2, s].astype(F32)
        return lo.astype(BF16), hi.astype(BF16)

    last, stay = [], []
    for n, (p, first, width) in enumerate(CHUNKS):
        cols = pl.ds(first, width)
        target = dev(yhh=yl, yll=1 - yl) if p else dev(yhh=yl)
        src, dst = fin.at[p, :, cols], yr.at[yh, :, cols]
        last.append(remote(src, dst, target, yssem.at[n], yrsem.at[yh, n]))
        stay.append(pltpu.make_async_copy(src, dst, yrsem.at[yh, n]))

    def send_fin(n):
        if CHUNKS[n][0] == 1:
            last[n].start()
            return

        @pl.when(yh != yl)
        def _():
            last[n].start()

        @pl.when(yh == yl)
        def _():
            stay[n].start()

    def hid_in(h, r):
        if r == 3:
            for s in range(2):
                f_p[h][s].wait_recv()
                f_m[h][s].wait_recv()
        else:
            copies = (a_p[h], b_p[h]) if r == 2 else (a_m[h], b_m[h])
            i = 1 if r == 2 else 0
            for copy in copies:
                copy[i].wait_recv()

    def forward(h, s):
        src_p, src_m = (b_p, b_m) if s else (a_p, a_m)
        src_p[h][0].wait_recv()
        start(f_p[h][s])
        src_m[h][1].wait_recv()
        start(f_m[h][s])

    def send_b(h):
        b_y[h].wait_recv()
        for i in range(2):
            start(b_p[h][i])
            start(b_m[h][1 - i])

    def g_in(r):
        g_y[r, 0].wait_recv()
        g_y[r, 1].wait_recv()

    def w_in(k):
        w_y[k].wait_recv()
        start(w_z[k])
        start(w_c[k])

    def w_near(k):
        w_z[k].wait_recv()
        start(w_d[k])
        turn(c, 1 - e, k)

    def w_core(k):
        w_c[k].wait_recv()
        turn(1 - c, e, k)

    def w_core_near(k):
        w_d[k].wait_recv()
        turn(1 - c, 1 - e, k)

    hg_own()
    w_in(0)
    forward(0, 0)
    send_b(0)
    flip(0, 0)
    wg_add(0, 0, 0, 256, True)
    w_in(1)
    turn(c, e, 0)
    turn(c, e, 1)
    forward(0, 1)
    for i in range(2):
        start(a_p[1][i])
        start(a_m[1][1 - i])
    w_in(2)
    w_near(0)
    w_core(0)
    turn(c, e, 2)
    hid_in(0, 1)
    hid_in(0, 2)
    flip(0, 1)
    flip(0, 2)
    wg_add(0, 0, 256, 512, False)
    w_in(3)
    w_near(1)
    hid_in(0, 3)
    flip(0, 3)
    wg_add(0, 0, 768, 256, False)
    cc_send(OWN, 0)
    turn(c, e, 3)
    w_core(1)
    forward(1, 0)
    send_b(1)
    w_near(2)
    reducer(0, z_own, 0)
    flip(1, 0)
    wg_add(0, 1, 0, 256, True)
    g_in(3)
    wg_add(1, 0, 768, 256, True)
    w_core(2)
    w_core(3)
    w_core_near(0)
    w_core_near(1)
    w_near(3)
    w_core_near(2)
    reducer(0, z_own, 1)
    w_core_near(3)
    hg_other(3)
    forward(1, 1)
    x_far(1)
    g_in(1)
    hg_other(1)
    reducer(0, z_own, 2)
    hid_in(1, 1)
    hid_in(1, 2)
    flip(1, 1)
    flip(1, 2)
    wg_add(0, 1, 256, 512, False)
    g_y[2, 0].wait_recv()
    hg_other(2, 1)
    x_direct(1)
    hid_in(1, 3)
    flip(1, 3)
    wg_add(0, 1, 768, 256, False)
    cc_send(OWN, 1)
    reducer(0, z_own, 3)
    g_y[2, 1].wait_recv()
    hg_other(2, 0)
    wg_add(1, 0, 256, 512, False)
    x_summed(1)
    x_far(0)
    x_direct(0)
    wg_add(1, 1, 256, 768, True)
    reducer(1, z_own, 0)
    reducer(0, z_own, 4)
    g_in(0)
    for h in range(2):
        wg_add(1, h, 0, 256, False)
        cc_send(PAIR, h)
    reducer(1, z_own, 1)
    hg_other(0)
    z_other(0)
    reducer(1, z_own, 2)
    z_other(1)
    lo, hi = x_total(1)
    yos[:, left] = lo
    yos[:, right] = hi
    start(o_y)
    reducer(1, z_own, 3)
    z_other(2)
    x_summed(0)
    reducer(1, z_own, 4)
    z_other(3)
    z_other(4)
    lo, hi = x_total(0)
    os[:, left] = lo
    os[:, right] = hi
    put_mine = local(os, out_ref.at[:, mine], 5)
    o_y.wait_recv()

    def arrived(slot, chunks):
        for n in chunks:
            _, first, width = CHUNKS[n]
            part = yr.at[slot, :, pl.ds(first, width)]
            pltpu.make_async_copy(part, part, yrsem.at[slot, n]).wait()

    @pl.when(yh == yl)
    def _():
        arrived(0, OWN)
        arrived(1, OWN)

    @pl.when(yh != yl)
    def _():
        arrived(0, PAIR)
        arrived(1, PAIR)
        for n in OWN:
            last[n].wait_send()

    for n in PAIR:
        last[n].wait_send()
    for copy in sent:
        copy.wait_send()
    put_mine.wait()


def hand_over(
    out_ref, yr_ref, out, gq, gk, gv, out_buf, yr_buf, g_buf, into, away
):
    yr_load = pltpu.make_async_copy(yr_ref, yr_buf, into.at[4])
    yr_load.start()
    loads, stores = [], []
    for i in range(4):
        part = pl.ds(i * 32, 32)
        loads.append(pltpu.make_async_copy(out_ref.at[part], out_buf.at[part], into.at[i]))
        stores.append(pltpu.make_async_copy(out_buf.at[part], out.at[part], away.at[i]))
    for load in loads:
        load.start()
    yr_load.wait()
    g_buf[...] = yr_buf[0].astype(F32) + yr_buf[1].astype(F32)
    for i, (ref, first, width) in enumerate(((gq, 0, CQ), (gk, CQ, CK), (gv, CQ + CK, CK))):
        stores.append(pltpu.make_async_copy(g_buf.at[:, pl.ds(first, width)], ref, away.at[4 + i]))
        stores[-1].start()
    for load, store in zip(loads, stores):
        load.wait()
        store.start()
    for store in stores:
        store.wait()


N_SEM = 112


def local_step(*args):
    scratch = [
        pltpu.VMEM((2, 8, 1024, T), BF16),
        pltpu.VMEM((2, 8, T, T), BF16),
        pltpu.VMEM((1024, C), BF16),
        pltpu.VMEM((1024, C), BF16),
        pltpu.VMEM((H, 1024), BF16),
        pltpu.VMEM((H, C), BF16),
        pltpu.VMEM((C, H), BF16),
        pltpu.VMEM((512, C), BF16),
        pltpu.VMEM((1024, H), F32),
        pltpu.VMEM((2, H, C), F32),
        pltpu.VMEM((2, 1024, C), BF16),
        pltpu.VMEM((2, 1024, C), BF16),
        pltpu.VMEM((2, 3, 2, T, HH), BF16),
        pltpu.VMEM((2, 3, 2, T, HH), BF16),
        pltpu.VMEM((2, 2, 448, C), BF16),
        pltpu.VMEM((2, 2, 448, C), BF16),
        pltpu.VMEM((2, T, C), BF16),
        pltpu.VMEM((T, H), BF16),
        pltpu.VMEM((T, H), BF16),
        pltpu.SemaphoreType.DMA((11,)),
        pltpu.SemaphoreType.DMA((N_SEM,)),
        pltpu.SemaphoreType.DMA((N_SEM,)),
        pltpu.SemaphoreType.DMA((len(CHUNKS),)),
        pltpu.SemaphoreType.DMA((2, len(CHUNKS))),
    ]
    anywhere = pl.BlockSpec(memory_space=pl.ANY)
    shapes = [((T, D), BF16), ((T, CQ), F32), ((T, CK), F32), ((T, CK), F32)]
    out_shape = tuple(jax.ShapeDtypeStruct(*shape) for shape in shapes)
    terms = jax.ShapeDtypeStruct((2, T, C), BF16)
    results = pl.pallas_call(
        kernel,
        out_shape=(out_shape[0], terms),
        in_specs=[anywhere] * 7,
        out_specs=(anywhere, anywhere),
        scratch_shapes=scratch,
        compiler_params=pltpu.CompilerParams(
            collective_id=0, has_side_effects=True, vmem_limit_bytes=67043328
        ),
    )(*args)
    return pl.pallas_call(
        hand_over,
        out_shape=out_shape,
        in_specs=[anywhere] * 2,
        out_specs=(anywhere,) * 4,
        scratch_shapes=[
            pltpu.VMEM((T, D), BF16),
            pltpu.VMEM((2, T, C), BF16),
            pltpu.VMEM((T, C), F32),
            pltpu.SemaphoreType.DMA((5,)),
            pltpu.SemaphoreType.DMA((7,)),
        ],
        cost_estimate=pl.CostEstimate(flops=0, bytes_accessed=3 << 20, transcendentals=0),
    )(*results)


def solution(mesh):
    both = P(("dp", "tp"), None)
    split = P("dp", "tp")
    return jax.shard_map(
        local_step,
        mesh=mesh,
        in_specs=(both, split, split, split, P(None, "tp"), P(None, "tp"), P(None, "tp")),
        out_specs=(both, split, split, split),
        check_vma=False,
    )
```

```python
import jax
import jax.numpy as jnp
from jax import lax
from jax.experimental import pallas as pl
from jax.experimental.pallas import tpu as pltpu
from jax.sharding import PartitionSpec as P

MESH = pl.DeviceIdType.MESH
BF16 = jnp.bfloat16
F32 = jnp.float32
T = 128
D = 4096
H = 2048
HH = 1024
CQ = 512
CK = 128
C = 768
CHUNKS = ((0, 0, 384), (0, 384, 384), (1, 0, 256), (1, 256, 256), (1, 512, 128), (1, 640, 128))
OWN = (0, 1)
POS = {(0, 0): 0, (0, 1): 1, (1, 0): 2, (2, 0): 3, (1, 1): 4, (2, 1): 5, (3, 0): 6, (3, 1): 7}
PAIR = (2, 3, 4, 5)


def nt(left, right):
    return lax.dot_general(left, right, (((1,), (1,)), ((), ())), preferred_element_type=F32)


def tn(left, right):
    return lax.dot_general(left, right, (((0,), (0,)), ((), ())), preferred_element_type=F32)


def kernel(
    hidden_ref,
    q_ref,
    k_ref,
    v_ref,
    wq_ref,
    wk_ref,
    wv_ref,
    out_ref,
    yr,
    hid,
    hsend,
    gown,
    goth,
    wh,
    woth,
    wt,
    wsend,
    hg,
    wg,
    ccs,
    ccr,
    xs,
    xr,
    zs,
    zr,
    fin,
    yos,
    os,
    lsem,
    ssem,
    rsem,
    yssem,
    yrsem,
):
    dp = lax.axis_index("dp")
    tp = lax.axis_index("tp")
    c = lax.rem(dp, 2)
    z = lax.rem(dp // 2, 8)
    yh = dp // 16
    yl = lax.rem(tp, 2)
    x = tp // 2
    e = lax.rem(z, 2)

    def dev(xx=None, yhh=None, yll=None, zz=None, cc=None):
        xx = x if xx is None else xx
        yhh = yh if yhh is None else yhh
        yll = yl if yll is None else yll
        zz = z if zz is None else zz
        cc = c if cc is None else cc
        return (yhh * 16 + zz * 2 + cc, xx * 2 + yll)

    XP = dev(xx=lax.rem(x + 1, 4))
    XM = dev(xx=lax.rem(x + 3, 4))
    YI = dev(yll=1 - yl)
    YO = dev(yhh=1 - yh, yll=1 - yl)
    Y2 = dev(yhh=1 - yh)
    ZP = dev(zz=lax.rem(z + 1, 8))
    ZM = dev(zz=lax.rem(z + 7, 8))
    ZX = dev(zz=z + 1 - 2 * e)
    CC = dev(cc=1 - c)

    counter = [0]
    sent = []

    def remote(src, dst, target, send=None, recv=None):
        if send is None:
            i = counter[0]
            counter[0] += 1
            send, recv = ssem.at[i], rsem.at[i]
        copy = pltpu.make_async_remote_copy(
            src_ref=src, dst_ref=dst, send_sem=send, recv_sem=recv, device_id=target, device_id_type=MESH
        )
        return copy

    def start(copy):
        copy.start()
        if not any(copy is one for one in sent):
            sent.append(copy)

    barrier = pltpu.get_barrier_semaphore()
    for target in (XP, XM, YI, YO, Y2, ZP, ZM, CC):
        pl.semaphore_signal(barrier, inc=1, device_id=target, device_id_type=MESH)

    def local(src, dst, i):
        copy = pltpu.make_async_copy(src, dst, lsem.at[i])
        copy.start()
        return copy

    mine = pl.ds(pl.multiple_of(yl * H, H), H)
    other = pl.ds(pl.multiple_of((1 - yl) * H, H), H)
    for h in range(2):
        for zz in range(8):
            first = pl.multiple_of(yl * H + (2 * zz + h) * T, T)
            local(hidden_ref.at[:, pl.ds(first, T)], hid.at[h, zz, pl.ds(0, T)], 0 if h == 0 else 10)
    for h in range(2):
        for zz in range(8):
            first = pl.multiple_of((1 - yl) * H + (2 * zz + h) * T, T)
            local(hidden_ref.at[:, pl.ds(first, T)], hsend.at[h, zz], 1)
    wrow = c * 1024 + e * 512
    wrows = pl.ds(pl.multiple_of((1 - yl) * H + wrow, 512), 512)
    local(wq_ref.at[wrows], wsend.at[:, pl.ds(0, CQ)], 2)
    local(wk_ref.at[wrows], wsend.at[:, pl.ds(CQ, CK)], 2)
    local(wv_ref.at[wrows], wsend.at[:, pl.ds(CQ + CK, CK)], 2)
    for r, off in enumerate((0, 1, 3, 2)):
        for s in range(2):
            block = lax.rem(x + off, 4) * 2 + (yl if s == 0 else 1 - yl)
            src = pl.ds(pl.multiple_of(block * T, T), T)
            dst = pl.ds(POS[r, s] * T, T)
            local(q_ref.at[src], gown.at[dst, pl.ds(0, CQ)], 3)
            local(k_ref.at[src], gown.at[dst, pl.ds(CQ, CK)], 3)
            local(v_ref.at[src], gown.at[dst, pl.ds(CQ + CK, CK)], 3)
    local(wq_ref.at[mine], wh.at[:, pl.ds(0, CQ)], 4)
    local(wk_ref.at[mine], wh.at[:, pl.ds(CQ, CK)], 4)
    local(wv_ref.at[mine], wh.at[:, pl.ds(CQ + CK, CK)], 4)

    def wait_local(buffer, i):
        pltpu.make_async_copy(buffer, buffer, lsem.at[i]).wait()

    pl.semaphore_wait(barrier, 8)

    def rows(r, s, half=None):
        first = POS[r, s] * T
        return pl.ds(first, T) if half is None else pl.ds(first + half * 64, 64)

    def piece(h, r, s, i):
        return hid.at[h, :, rows(r, s, i)]

    both = range(2)
    a_p = [[remote(piece(h, 0, 0, i), piece(h, 2, 0, i), XP) for i in both] for h in both]
    a_m = [[remote(piece(h, 0, 0, i), piece(h, 1, 0, i), XM) for i in both] for h in both]
    b_y = [remote(hsend.at[h], hid.at[h, :, rows(0, 1)], YI) for h in both]
    b_p = [[remote(piece(h, 0, 1, i), piece(h, 2, 1, i), XP) for i in both] for h in both]
    b_m = [[remote(piece(h, 0, 1, i), piece(h, 1, 1, i), XM) for i in both] for h in both]
    f_p = [[remote(piece(h, 2, s, 0), piece(h, 3, s, 0), XP) for s in both] for h in both]
    f_m = [[remote(piece(h, 1, s, 1), piece(h, 3, s, 1), XM) for s in both] for h in both]
    g_y = {
        (r, s): remote(gown.at[rows(r, s)], goth.at[rows(r, 1 - s)], YI) for r in (3, 1, 2, 0) for s in range(2)
    }

    def wpiece(cc, ee, k):
        return pl.ds(pl.multiple_of(cc * 1024 + ee * 512 + k * 128, 128), 128)

    w_y = [remote(wsend.at[pl.ds(128 * k, 128)], woth.at[wpiece(c, e, k)], YO) for k in range(4)]
    w_z = [remote(woth.at[wpiece(c, e, k)], woth.at[wpiece(c, e, k)], ZX) for k in range(4)]
    w_c = [remote(woth.at[wpiece(c, e, k)], woth.at[wpiece(c, e, k)], CC) for k in range(4)]
    w_d = [remote(woth.at[wpiece(c, 1 - e, k)], woth.at[wpiece(c, 1 - e, k)], CC) for k in range(4)]
    xc = {
        (d, b, s): remote(xs.at[d, b, s], xr.at[d, b, s], XP if d == 0 else XM)
        for d in range(2)
        for b in range(3)
        for s in range(2)
    }
    o_y = remote(yos, out_ref.at[:, mine], YI)
    cc_copy = []
    for n, (p, first, width) in enumerate(CHUNKS):
        cols = pl.ds(first, width)
        cc_copy.append(remote(ccs.at[p, :, cols], ccr.at[p, :, cols], CC))
    steps = (pl.ds(0, 64), pl.ds(64, 128), pl.ds(192, 128), pl.ds(320, 128))
    zc = {}
    for n, (p, first, width) in enumerate(CHUNKS):
        cols = pl.ds(first, width)
        for d in range(2):
            for i in range(4):
                part = (p, d, steps[i], cols)
                zc[n, d, i] = remote(zs.at[part], zr.at[part], ZP if d == 0 else ZM)

    wait_local(hid.at[0, :, pl.ds(0, T)], 0)
    for i in range(2):
        start(a_p[0][i])
        start(a_m[0][1 - i])
    wait_local(hsend, 1)
    start(b_y[0])
    wait_local(wsend, 2)
    for k in range(4):
        start(w_y[k])
    wait_local(gown, 3)
    start(g_y[3, 0])
    start(g_y[3, 1])
    start(b_y[1])
    for s in range(2):
        start(g_y[1, s])
        start(g_y[2, s])
    start(g_y[0, 0])
    start(g_y[0, 1])
    wait_local(hid.at[1, :, pl.ds(0, T)], 10)
    wait_local(wh.at[:, pl.ds(0, C)], 4)

    def hg_own():
        def step(n, carry):
            cols = pl.ds(pl.multiple_of(n * 256, 256), 256)
            w = wh[cols, :C]
            for m in range(2):
                hg[pl.ds(m * 512, 512), cols] = nt(gown[pl.ds(m * 512, 512), :], w)
            return carry

        lax.fori_loop(0, 8, step, 0)

    def turn(cc, ee, k):
        piece = wpiece(cc, ee, k)
        wt[:, piece] = woth[piece, :].T

    def hg_other(group):
        block = pl.ds(group * 256, 256)

        def step(n, carry):
            cols = pl.ds(pl.multiple_of(n * 512, 512), 512)
            hg[block, cols] += jnp.dot(goth[block, :], wt[:, cols], preferred_element_type=F32)
            return carry

        lax.fori_loop(0, 4, step, 0)

    def flip(h, r):
        def step(zz, carry):
            dst = pl.ds(pl.multiple_of(h * 1024 + zz * T, T), T)
            block = pl.ds(r * 256, 256)
            wh[dst, block] = hid[h, zz, block, :].T
            return carry

        lax.fori_loop(0, 8, step, 0)

    def wg_add(pair, h, first, depth, fresh):
        g = goth if pair else gown
        toks = pl.ds(first, depth)

        def step(m, carry):
            block = pl.ds(pl.multiple_of(h * 1024 + m * 512, 512), 512)
            part = jnp.dot(wh[block, toks], g[toks, :], preferred_element_type=F32)
            wg[pair, block, :] = part if fresh else wg[pair, block, :] + part
            return carry

        lax.fori_loop(0, 2, step, 0)

    def cc_send(chunks, h):
        @pl.when(c != h)
        def _():
            for n in chunks:
                p, first, width = CHUNKS[n]
                cols = pl.ds(first, width)
                for m in range(4):
                    src = pl.ds(h * 1024 + m * 256, 256)
                    ccs[p, pl.ds(m * 256, 256), cols] = wg[p, src, cols].astype(BF16)
                start(cc_copy[n])

    def pair_sum(n, zz, start_row=0, size=T):
        p, first, width = CHUNKS[n]
        cols = pl.ds(first, width)
        src = pl.ds(pl.multiple_of(c * 1024 + zz * T + start_row, size), size)
        dst = pl.ds(pl.multiple_of(zz * T + start_row, size), size)
        return wg[p, src, cols] + ccr[p, dst, cols].astype(F32)

    def z_own(i):
        for n in OWN:
            z_any(n, i)

    def z_other(i):
        for n in PAIR:
            z_any(n, i)

    def z_any(n, i):
        if i == 0:
            cc_copy[n].wait_recv()
        if i < 4:
            z_step(n, i)
        else:
            z_last(n)
            send_fin(n)

    def reducer(h, work, *args):
        @pl.when(c == h)
        def _():
            work(*args)

    def z_step(n, i):
        p, first, width = CHUNKS[n]
        cols = pl.ds(first, width)
        if i == 0:
            far = lax.rem(z + 4, 8)
            for d in range(2):
                zs[p, d, steps[0], cols] = pair_sum(n, far, d * 64, 64).astype(BF16)
                start(zc[n, d, 0])
        for d in range(2) if i else ():
            zz = lax.rem(z + 4 - i, 8) if d == 0 else lax.rem(z + 4 + i, 8)
            zc[n, d, i - 1].wait_recv()
            came = zr[p, d, steps[i - 1], cols].astype(F32)
            if i == 1:
                for half in range(2):
                    part = pair_sum(n, zz, half * 64, 64)
                    if half == d:
                        part = part + came
                    zs[p, d, pl.ds(64 + half * 64, 64), cols] = part.astype(BF16)
            else:
                zs[p, d, steps[i], cols] = (pair_sum(n, zz) + came).astype(BF16)
            start(zc[n, d, i])

    def z_last(n):
        p, first, width = CHUNKS[n]
        cols = pl.ds(first, width)
        for d in range(2):
            zc[n, d, 3].wait_recv()
        came = zr[p, 0, steps[3], cols].astype(F32) + zr[p, 1, steps[3], cols].astype(F32)
        fin[p, :, cols] = (pair_sum(n, z) + came).astype(BF16)

    left, right = pl.ds(0, HH), pl.ds(HH, HH)

    def x_far(s):
        block = pl.ds(3 * 256 + s * T, T)
        xs[0, 0, s] = hg[block, left].astype(BF16)
        start(xc[0, 0, s])
        xs[1, 0, s] = hg[block, right].astype(BF16)
        start(xc[1, 0, s])

    def x_direct(s):
        xs[0, 1, s] = hg[rows(1, s), right].astype(BF16)
        start(xc[0, 1, s])
        xs[1, 1, s] = hg[rows(2, s), left].astype(BF16)
        start(xc[1, 1, s])

    def x_summed(s):
        xc[0, 0, s].wait_recv()
        xs[0, 2, s] = (hg[rows(1, s), left] + xr[0, 0, s].astype(F32)).astype(BF16)
        start(xc[0, 2, s])
        xc[1, 0, s].wait_recv()
        xs[1, 2, s] = (hg[rows(2, s), right] + xr[1, 0, s].astype(F32)).astype(BF16)
        start(xc[1, 2, s])

    def x_total(s):
        for d in range(2):
            xc[d, 1, s].wait_recv()
            xc[d, 2, s].wait_recv()
        block = pl.ds(s * T, T)
        lo = hg[block, left] + xr[0, 2, s].astype(F32) + xr[1, 1, s].astype(F32)
        hi = hg[block, right] + xr[0, 1, s].astype(F32) + xr[1, 2, s].astype(F32)
        return lo.astype(BF16), hi.astype(BF16)

    last, stay = [], []
    for n, (p, first, width) in enumerate(CHUNKS):
        cols = pl.ds(first, width)
        target = dev(yhh=yl, yll=1 - yl) if p else dev(yhh=yl)
        src, dst = fin.at[p, :, cols], yr.at[yh, :, cols]
        last.append(remote(src, dst, target, yssem.at[n], yrsem.at[yh, n]))
        stay.append(pltpu.make_async_copy(src, dst, yrsem.at[yh, n]))

    def send_fin(n):
        if CHUNKS[n][0] == 1:
            last[n].start()
            return

        @pl.when(yh != yl)
        def _():
            last[n].start()

        @pl.when(yh == yl)
        def _():
            stay[n].start()

    def hid_in(h, group):
        if group == 3:
            for s in range(2):
                f_p[h][s].wait_recv()
                f_m[h][s].wait_recv()
        elif group == 1:
            a_p[h][1].wait_recv()
            a_m[h][0].wait_recv()
        else:
            b_p[h][1].wait_recv()
            b_m[h][0].wait_recv()

    def forward(h, s):
        src_p, src_m = (b_p, b_m) if s else (a_p, a_m)
        src_p[h][0].wait_recv()
        start(f_p[h][s])
        src_m[h][1].wait_recv()
        start(f_m[h][s])

    def send_b(h):
        b_y[h].wait_recv()
        for i in range(2):
            start(b_p[h][i])
            start(b_m[h][1 - i])

    def g_in(group):
        pairs = ((0, 0), (0, 1)), ((1, 1), (2, 1)), ((1, 0), (2, 0)), ((3, 0), (3, 1))
        for pair in pairs[group]:
            g_y[pair].wait_recv()

    def w_in(k):
        w_y[k].wait_recv()
        start(w_z[k])
        start(w_c[k])

    def w_near(k):
        w_z[k].wait_recv()
        start(w_d[k])
        turn(c, 1 - e, k)

    def w_core(k):
        w_c[k].wait_recv()
        turn(1 - c, e, k)

    def w_core_near(k):
        w_d[k].wait_recv()
        turn(1 - c, 1 - e, k)

    hg_own()
    forward(0, 0)
    send_b(0)
    w_in(0)
    flip(0, 0)
    wg_add(0, 0, 0, 256, True)
    w_in(1)
    turn(c, e, 0)
    turn(c, e, 1)
    hid_in(0, 1)
    flip(0, 1)
    forward(0, 1)
    for i in range(2):
        start(a_p[1][i])
        start(a_m[1][1 - i])
    w_in(2)
    w_near(0)
    w_core(0)
    turn(c, e, 2)
    hid_in(0, 2)
    flip(0, 2)
    wg_add(0, 0, 256, 512, False)
    w_in(3)
    w_near(1)
    hid_in(0, 3)
    flip(0, 3)
    wg_add(0, 0, 768, 256, False)
    cc_send(OWN, 0)
    turn(c, e, 3)
    w_core(1)
    forward(1, 0)
    send_b(1)
    w_near(2)
    reducer(0, z_own, 0)
    flip(1, 0)
    wg_add(0, 1, 0, 256, True)
    g_in(3)
    wg_add(1, 0, 768, 256, True)
    w_core(2)
    w_core(3)
    w_core_near(0)
    w_core_near(1)
    w_near(3)
    w_core_near(2)
    reducer(0, z_own, 1)
    w_core_near(3)
    hg_other(3)
    hid_in(1, 1)
    flip(1, 1)
    wg_add(0, 1, 256, 256, False)
    forward(1, 1)
    x_far(1)
    g_in(2)
    hg_other(2)
    x_direct(1)
    reducer(0, z_own, 2)
    hid_in(1, 2)
    flip(1, 2)
    wg_add(0, 1, 512, 256, False)
    hid_in(1, 3)
    flip(1, 3)
    wg_add(0, 1, 768, 256, False)
    cc_send(OWN, 1)
    reducer(0, z_own, 3)
    g_in(1)
    hg_other(1)
    wg_add(1, 0, 256, 512, False)
    x_summed(1)
    x_far(0)
    x_direct(0)
    wg_add(1, 1, 256, 768, True)
    reducer(1, z_own, 0)
    reducer(0, z_own, 4)
    g_in(0)
    for h in range(2):
        wg_add(1, h, 0, 256, False)
        cc_send(PAIR, h)
    reducer(1, z_own, 1)
    hg_other(0)
    z_other(0)
    reducer(1, z_own, 2)
    z_other(1)
    lo, hi = x_total(1)
    yos[:, left] = lo
    yos[:, right] = hi
    start(o_y)
    reducer(1, z_own, 3)
    z_other(2)
    x_summed(0)
    reducer(1, z_own, 4)
    z_other(3)
    z_other(4)
    lo, hi = x_total(0)
    os[:, left] = lo
    os[:, right] = hi
    put_mine = local(os, out_ref.at[:, mine], 5)
    o_y.wait_recv()

    def arrived(slot, chunks):
        for n in chunks:
            _, first, width = CHUNKS[n]
            part = yr.at[slot, :, pl.ds(first, width)]
            pltpu.make_async_copy(part, part, yrsem.at[slot, n]).wait()

    @pl.when(yh == yl)
    def _():
        arrived(0, OWN)
        arrived(1, OWN)

    @pl.when(yh != yl)
    def _():
        arrived(0, PAIR)
        arrived(1, PAIR)
        for n in OWN:
            last[n].wait_send()

    for n in PAIR:
        last[n].wait_send()
    for copy in sent:
        copy.wait_send()
    put_mine.wait()


def hand_over(
    out_ref, yr_ref, out, gq, gk, gv, out_buf, yr_buf, g_buf, into, away
):
    yr_load = pltpu.make_async_copy(yr_ref, yr_buf, into.at[4])
    yr_load.start()
    loads, stores = [], []
    for i in range(4):
        part = pl.ds(i * 32, 32)
        loads.append(pltpu.make_async_copy(out_ref.at[part], out_buf.at[part], into.at[i]))
        stores.append(pltpu.make_async_copy(out_buf.at[part], out.at[part], away.at[i]))
    for load in loads:
        load.start()
    yr_load.wait()
    g_buf[...] = yr_buf[0].astype(F32) + yr_buf[1].astype(F32)
    for i, (ref, first, width) in enumerate(((gq, 0, CQ), (gk, CQ, CK), (gv, CQ + CK, CK))):
        stores.append(pltpu.make_async_copy(g_buf.at[:, pl.ds(first, width)], ref, away.at[4 + i]))
        stores[-1].start()
    for load, store in zip(loads, stores):
        load.wait()
        store.start()
    for store in stores:
        store.wait()


N_SEM = 120


def local_step(*args):
    scratch = [
        pltpu.VMEM((2, 8, 1024, T), BF16),
        pltpu.VMEM((2, 8, T, T), BF16),
        pltpu.VMEM((1024, C), BF16),
        pltpu.VMEM((1024, C), BF16),
        pltpu.VMEM((H, 1024), BF16),
        pltpu.VMEM((H, C), BF16),
        pltpu.VMEM((C, H), BF16),
        pltpu.VMEM((512, C), BF16),
        pltpu.VMEM((1024, H), F32),
        pltpu.VMEM((2, H, C), F32),
        pltpu.VMEM((2, 1024, C), BF16),
        pltpu.VMEM((2, 1024, C), BF16),
        pltpu.VMEM((2, 3, 2, T, HH), BF16),
        pltpu.VMEM((2, 3, 2, T, HH), BF16),
        pltpu.VMEM((2, 2, 448, C), BF16),
        pltpu.VMEM((2, 2, 448, C), BF16),
        pltpu.VMEM((2, T, C), BF16),
        pltpu.VMEM((T, H), BF16),
        pltpu.VMEM((T, H), BF16),
        pltpu.SemaphoreType.DMA((11,)),
        pltpu.SemaphoreType.DMA((N_SEM,)),
        pltpu.SemaphoreType.DMA((N_SEM,)),
        pltpu.SemaphoreType.DMA((len(CHUNKS),)),
        pltpu.SemaphoreType.DMA((2, len(CHUNKS))),
    ]
    anywhere = pl.BlockSpec(memory_space=pl.ANY)
    shapes = [((T, D), BF16), ((T, CQ), F32), ((T, CK), F32), ((T, CK), F32)]
    out_shape = tuple(jax.ShapeDtypeStruct(*shape) for shape in shapes)
    terms = jax.ShapeDtypeStruct((2, T, C), BF16)
    results = pl.pallas_call(
        kernel,
        out_shape=(out_shape[0], terms),
        in_specs=[anywhere] * 7,
        out_specs=(anywhere, anywhere),
        scratch_shapes=scratch,
        compiler_params=pltpu.CompilerParams(
            collective_id=0, has_side_effects=True, vmem_limit_bytes=67043328
        ),
    )(*args)
    return pl.pallas_call(
        hand_over,
        out_shape=out_shape,
        in_specs=[anywhere] * 2,
        out_specs=(anywhere,) * 4,
        scratch_shapes=[
            pltpu.VMEM((T, D), BF16),
            pltpu.VMEM((2, T, C), BF16),
            pltpu.VMEM((T, C), F32),
            pltpu.SemaphoreType.DMA((5,)),
            pltpu.SemaphoreType.DMA((7,)),
        ],
        cost_estimate=pl.CostEstimate(flops=0, bytes_accessed=3 << 20, transcendentals=0),
    )(*results)


def solution(mesh):
    both = P(("dp", "tp"), None)
    split = P("dp", "tp")
    return jax.shard_map(
        local_step,
        mesh=mesh,
        in_specs=(both, split, split, split, P(None, "tp"), P(None, "tp"), P(None, "tp")),
        out_specs=(both, split, split, split),
        check_vma=False,
    )
```

```python
import jax
import jax.numpy as jnp
from jax import lax
from jax.experimental import pallas as pl
from jax.experimental.pallas import tpu as pltpu
from jax.sharding import PartitionSpec as P

MESH = pl.DeviceIdType.MESH
BF16 = jnp.bfloat16
F32 = jnp.float32
T = 128
D = 4096
H = 2048
HH = 1024
CQ = 512
CK = 128
C = 768
CHUNKS = ((0, 0, 384), (0, 384, 384), (1, 0, 256), (1, 256, 256), (1, 512, 256))
OWN = (0, 1)
PAIR = (2, 3, 4)


def nt(left, right):
    return lax.dot_general(left, right, (((1,), (1,)), ((), ())), preferred_element_type=F32)


def tn(left, right):
    return lax.dot_general(left, right, (((0,), (0,)), ((), ())), preferred_element_type=F32)


def kernel(
    hidden_ref,
    q_ref,
    k_ref,
    v_ref,
    wq_ref,
    wk_ref,
    wv_ref,
    out_ref,
    yr,
    hid,
    hsend,
    gown,
    goth,
    wh,
    woth,
    wt,
    wsend,
    hg,
    wg,
    ccs,
    ccr,
    xs,
    xr,
    zs,
    zr,
    fin,
    yos,
    os,
    lsem,
    ssem,
    rsem,
    yssem,
    yrsem,
):
    dp = lax.axis_index("dp")
    tp = lax.axis_index("tp")
    c = lax.rem(dp, 2)
    z = lax.rem(dp // 2, 8)
    yh = dp // 16
    yl = lax.rem(tp, 2)
    x = tp // 2
    e = lax.rem(z, 2)

    def dev(xx=None, yhh=None, yll=None, zz=None, cc=None):
        xx = x if xx is None else xx
        yhh = yh if yhh is None else yhh
        yll = yl if yll is None else yll
        zz = z if zz is None else zz
        cc = c if cc is None else cc
        return (yhh * 16 + zz * 2 + cc, xx * 2 + yll)

    XP = dev(xx=lax.rem(x + 1, 4))
    XM = dev(xx=lax.rem(x + 3, 4))
    YI = dev(yll=1 - yl)
    YO = dev(yhh=1 - yh, yll=1 - yl)
    Y2 = dev(yhh=1 - yh)
    ZP = dev(zz=lax.rem(z + 1, 8))
    ZM = dev(zz=lax.rem(z + 7, 8))
    ZX = dev(zz=z + 1 - 2 * e)
    CC = dev(cc=1 - c)

    counter = [0]
    sent = []

    def remote(src, dst, target, send=None, recv=None):
        if send is None:
            i = counter[0]
            counter[0] += 1
            send, recv = ssem.at[i], rsem.at[i]
        copy = pltpu.make_async_remote_copy(
            src_ref=src, dst_ref=dst, send_sem=send, recv_sem=recv, device_id=target, device_id_type=MESH
        )
        return copy

    def start(copy):
        copy.start()
        if not any(copy is one for one in sent):
            sent.append(copy)

    def local(src, dst, i):
        copy = pltpu.make_async_copy(src, dst, lsem.at[i])
        copy.start()
        return copy

    mine = pl.ds(pl.multiple_of(yl * H, H), H)
    other = pl.ds(pl.multiple_of((1 - yl) * H, H), H)
    for h in range(2):
        for zz in range(8):
            first = pl.multiple_of(yl * H + (2 * zz + h) * T, T)
            local(hidden_ref.at[:, pl.ds(first, T)], hid.at[h, zz, pl.ds(0, T)], 0 if h == 0 else 10)
    for h in range(2):
        for zz in range(8):
            first = pl.multiple_of((1 - yl) * H + (2 * zz + h) * T, T)
            local(hidden_ref.at[:, pl.ds(first, T)], hsend.at[h, zz], 1)
    wrow = c * 1024 + e * 512
    wrows = pl.ds(pl.multiple_of((1 - yl) * H + wrow, 512), 512)
    local(wq_ref.at[wrows], wsend.at[:, pl.ds(0, CQ)], 2)
    local(wk_ref.at[wrows], wsend.at[:, pl.ds(CQ, CK)], 2)
    local(wv_ref.at[wrows], wsend.at[:, pl.ds(CQ + CK, CK)], 2)
    for r, off in enumerate((0, 1, 3, 2)):
        for s in range(2):
            block = lax.rem(x + off, 4) * 2 + (yl if s == 0 else 1 - yl)
            src = pl.ds(pl.multiple_of(block * T, T), T)
            dst = pl.ds(r * 256 + s * T, T)
            local(q_ref.at[src], gown.at[dst, pl.ds(0, CQ)], 3)
            local(k_ref.at[src], gown.at[dst, pl.ds(CQ, CK)], 3)
            local(v_ref.at[src], gown.at[dst, pl.ds(CQ + CK, CK)], 3)
    local(wq_ref.at[mine], wh.at[:, pl.ds(0, CQ)], 4)
    local(wk_ref.at[mine], wh.at[:, pl.ds(CQ, CK)], 4)
    local(wv_ref.at[mine], wh.at[:, pl.ds(CQ + CK, CK)], 4)

    def wait_local(buffer, i):
        pltpu.make_async_copy(buffer, buffer, lsem.at[i]).wait()

    barrier = pltpu.get_barrier_semaphore()
    for target in (XP, XM, YI, YO, Y2, ZP, ZM, CC):
        pl.semaphore_signal(barrier, inc=1, device_id=target, device_id_type=MESH)
    pl.semaphore_wait(barrier, 8)

    def rows(r, s, half=None):
        first = r * 256 + s * T
        return pl.ds(first, T) if half is None else pl.ds(first + half * 64, 64)

    def piece(h, r, s, i):
        return hid.at[h, :, rows(r, s, i)]

    both = range(2)
    a_p = [[remote(piece(h, 0, 0, i), piece(h, 2, 0, i), XP) for i in both] for h in both]
    a_m = [[remote(piece(h, 0, 0, i), piece(h, 1, 0, i), XM) for i in both] for h in both]
    b_y = [remote(hsend.at[h], hid.at[h, :, rows(0, 1)], YI) for h in both]
    b_p = [[remote(piece(h, 0, 1, i), piece(h, 2, 1, i), XP) for i in both] for h in both]
    b_m = [[remote(piece(h, 0, 1, i), piece(h, 1, 1, i), XM) for i in both] for h in both]
    f_p = [[remote(piece(h, 2, s, 0), piece(h, 3, s, 0), XP) for s in both] for h in both]
    f_m = [[remote(piece(h, 1, s, 1), piece(h, 3, s, 1), XM) for s in both] for h in both]
    g_y = {
        (r, s): remote(gown.at[rows(r, s)], goth.at[rows(r, 1 - s)], YI) for r in (3, 1, 2, 0) for s in range(2)
    }

    def wpiece(cc, ee, k):
        return pl.ds(pl.multiple_of(cc * 1024 + ee * 512 + k * 128, 128), 128)

    w_y = [remote(wsend.at[pl.ds(128 * k, 128)], woth.at[wpiece(c, e, k)], YO) for k in range(4)]
    w_z = [remote(woth.at[wpiece(c, e, k)], woth.at[wpiece(c, e, k)], ZX) for k in range(4)]
    w_c = [remote(woth.at[wpiece(c, e, k)], woth.at[wpiece(c, e, k)], CC) for k in range(4)]
    w_d = [remote(woth.at[wpiece(c, 1 - e, k)], woth.at[wpiece(c, 1 - e, k)], CC) for k in range(4)]
    xc = {
        (d, b, s): remote(xs.at[d, b, s], xr.at[d, b, s], XP if d == 0 else XM)
        for d in range(2)
        for b in range(3)
        for s in range(2)
    }
    o_y = remote(yos, out_ref.at[:, mine], YI)
    cc_copy = []
    for n, (p, first, width) in enumerate(CHUNKS):
        cols = pl.ds(first, width)
        cc_copy.append(remote(ccs.at[p, :, cols], ccr.at[p, :, cols], CC))
    steps = (pl.ds(0, 64), pl.ds(64, 128), pl.ds(192, 128), pl.ds(320, 128))
    zc = {}
    for n, (p, first, width) in enumerate(CHUNKS):
        cols = pl.ds(first, width)
        for d in range(2):
            for i in range(4):
                part = (p, d, steps[i], cols)
                zc[n, d, i] = remote(zs.at[part], zr.at[part], ZP if d == 0 else ZM)

    wait_local(hid.at[0, :, pl.ds(0, T)], 0)
    for i in range(2):
        start(a_p[0][i])
        start(a_m[0][1 - i])
    wait_local(hsend, 1)
    start(b_y[0])
    wait_local(wsend, 2)
    for k in range(4):
        start(w_y[k])
    wait_local(gown, 3)
    for r in (3, 1, 2, 0):
        for s in (0, 1):
            start(g_y[r, s])
        if r == 3:
            start(b_y[1])
    wait_local(hid.at[1, :, pl.ds(0, T)], 10)
    wait_local(wh.at[:, pl.ds(0, C)], 4)

    def hg_own():
        def step(n, carry):
            cols = pl.ds(pl.multiple_of(n * 256, 256), 256)
            w = wh[cols, :C]
            for m in range(2):
                hg[pl.ds(m * 512, 512), cols] = nt(gown[pl.ds(m * 512, 512), :], w)
            return carry

        lax.fori_loop(0, 8, step, 0)

    def turn(cc, ee, k):
        piece = wpiece(cc, ee, k)
        wt[:, piece] = woth[piece, :].T

    def hg_other(r, s=None):
        block = pl.ds(r * 256, 256) if s is None else pl.ds(r * 256 + s * T, T)

        def step(n, carry):
            cols = pl.ds(pl.multiple_of(n * 512, 512), 512)
            hg[block, cols] += jnp.dot(goth[block, :], wt[:, cols], preferred_element_type=F32)
            return carry

        lax.fori_loop(0, 4, step, 0)

    def flip(h, r):
        def step(zz, carry):
            dst = pl.ds(pl.multiple_of(h * 1024 + zz * T, T), T)
            block = pl.ds(r * 256, 256)
            wh[dst, block] = hid[h, zz, block, :].T
            return carry

        lax.fori_loop(0, 8, step, 0)

    def wg_add(pair, h, first, depth, fresh):
        g = goth if pair else gown
        toks = pl.ds(first, depth)

        def step(m, carry):
            block = pl.ds(pl.multiple_of(h * 1024 + m * 512, 512), 512)
            part = jnp.dot(wh[block, toks], g[toks, :], preferred_element_type=F32)
            wg[pair, block, :] = part if fresh else wg[pair, block, :] + part
            return carry

        lax.fori_loop(0, 2, step, 0)

    def cc_send(chunks, h):
        @pl.when(c != h)
        def _():
            for n in chunks:
                p, first, width = CHUNKS[n]
                cols = pl.ds(first, width)
                for m in range(4):
                    src = pl.ds(h * 1024 + m * 256, 256)
                    ccs[p, pl.ds(m * 256, 256), cols] = wg[p, src, cols].astype(BF16)
                start(cc_copy[n])

    def pair_sum(n, zz, start_row=0, size=T):
        p, first, width = CHUNKS[n]
        cols = pl.ds(first, width)
        src = pl.ds(pl.multiple_of(c * 1024 + zz * T + start_row, size), size)
        dst = pl.ds(pl.multiple_of(zz * T + start_row, size), size)
        return wg[p, src, cols] + ccr[p, dst, cols].astype(F32)

    def z_own(i):
        for n in OWN:
            z_any(n, i)

    def z_other(i):
        for n in PAIR:
            z_any(n, i)

    def z_any(n, i):
        if i == 0:
            cc_copy[n].wait_recv()
        if i < 4:
            z_step(n, i)
        else:
            z_last(n)
            send_fin(n)

    def reducer(h, work, *args):
        @pl.when(c == h)
        def _():
            work(*args)

    def z_step(n, i):
        p, first, width = CHUNKS[n]
        cols = pl.ds(first, width)
        if i == 0:
            far = lax.rem(z + 4, 8)
            for d in range(2):
                zs[p, d, steps[0], cols] = pair_sum(n, far, d * 64, 64).astype(BF16)
                start(zc[n, d, 0])
        for d in range(2) if i else ():
            zz = lax.rem(z + 4 - i, 8) if d == 0 else lax.rem(z + 4 + i, 8)
            zc[n, d, i - 1].wait_recv()
            came = zr[p, d, steps[i - 1], cols].astype(F32)
            if i == 1:
                for half in range(2):
                    part = pair_sum(n, zz, half * 64, 64)
                    if half == d:
                        part = part + came
                    zs[p, d, pl.ds(64 + half * 64, 64), cols] = part.astype(BF16)
            else:
                zs[p, d, steps[i], cols] = (pair_sum(n, zz) + came).astype(BF16)
            start(zc[n, d, i])

    def z_last(n):
        p, first, width = CHUNKS[n]
        cols = pl.ds(first, width)
        for d in range(2):
            zc[n, d, 3].wait_recv()
        came = zr[p, 0, steps[3], cols].astype(F32) + zr[p, 1, steps[3], cols].astype(F32)
        fin[p, :, cols] = (pair_sum(n, z) + came).astype(BF16)

    left, right = pl.ds(0, HH), pl.ds(HH, HH)

    def x_far(s):
        block = pl.ds(3 * 256 + s * T, T)
        xs[0, 0, s] = hg[block, left].astype(BF16)
        start(xc[0, 0, s])
        xs[1, 0, s] = hg[block, right].astype(BF16)
        start(xc[1, 0, s])

    def x_direct(s):
        xs[0, 1, s] = hg[pl.ds(1 * 256 + s * T, T), right].astype(BF16)
        start(xc[0, 1, s])
        xs[1, 1, s] = hg[pl.ds(2 * 256 + s * T, T), left].astype(BF16)
        start(xc[1, 1, s])

    def x_summed(s):
        xc[0, 0, s].wait_recv()
        xs[0, 2, s] = (hg[pl.ds(1 * 256 + s * T, T), left] + xr[0, 0, s].astype(F32)).astype(BF16)
        start(xc[0, 2, s])
        xc[1, 0, s].wait_recv()
        xs[1, 2, s] = (hg[pl.ds(2 * 256 + s * T, T), right] + xr[1, 0, s].astype(F32)).astype(BF16)
        start(xc[1, 2, s])

    def x_total(s):
        for d in range(2):
            xc[d, 1, s].wait_recv()
            xc[d, 2, s].wait_recv()
        block = pl.ds(s * T, T)
        lo = hg[block, left] + xr[0, 2, s].astype(F32) + xr[1, 1, s].astype(F32)
        hi = hg[block, right] + xr[0, 1, s].astype(F32) + xr[1, 2, s].astype(F32)
        return lo.astype(BF16), hi.astype(BF16)

    last, stay = [], []
    for n, (p, first, width) in enumerate(CHUNKS):
        cols = pl.ds(first, width)
        target = dev(yhh=yl, yll=1 - yl) if p else dev(yhh=yl)
        src, dst = fin.at[p, :, cols], yr.at[yh, :, cols]
        last.append(remote(src, dst, target, yssem.at[n], yrsem.at[yh, n]))
        stay.append(pltpu.make_async_copy(src, dst, yrsem.at[yh, n]))

    def send_fin(n):
        if CHUNKS[n][0] == 1:
            last[n].start()
            return

        @pl.when(yh != yl)
        def _():
            last[n].start()

        @pl.when(yh == yl)
        def _():
            stay[n].start()

    def hid_in(h, r):
        if r == 3:
            for s in range(2):
                f_p[h][s].wait_recv()
                f_m[h][s].wait_recv()
        else:
            copies = (a_p[h], b_p[h]) if r == 2 else (a_m[h], b_m[h])
            i = 1 if r == 2 else 0
            for copy in copies:
                copy[i].wait_recv()

    def forward(h, s):
        src_p, src_m = (b_p, b_m) if s else (a_p, a_m)
        src_p[h][0].wait_recv()
        start(f_p[h][s])
        src_m[h][1].wait_recv()
        start(f_m[h][s])

    def send_b(h):
        b_y[h].wait_recv()
        for i in range(2):
            start(b_p[h][i])
            start(b_m[h][1 - i])

    def g_in(r):
        g_y[r, 0].wait_recv()
        g_y[r, 1].wait_recv()

    def w_in(k):
        w_y[k].wait_recv()
        start(w_z[k])
        start(w_c[k])

    def w_near(k):
        w_z[k].wait_recv()
        start(w_d[k])
        turn(c, 1 - e, k)

    def w_core(k):
        w_c[k].wait_recv()
        turn(1 - c, e, k)

    def w_core_near(k):
        w_d[k].wait_recv()
        turn(1 - c, 1 - e, k)

    hg_own()
    forward(0, 0)
    send_b(0)
    w_in(0)
    flip(0, 0)
    wg_add(0, 0, 0, 256, True)
    w_in(1)
    turn(c, e, 0)
    turn(c, e, 1)
    forward(0, 1)
    for i in range(2):
        start(a_p[1][i])
        start(a_m[1][1 - i])
    w_in(2)
    w_near(0)
    w_core(0)
    turn(c, e, 2)
    hid_in(0, 1)
    hid_in(0, 2)
    flip(0, 1)
    flip(0, 2)
    wg_add(0, 0, 256, 512, False)
    w_in(3)
    w_near(1)
    hid_in(0, 3)
    flip(0, 3)
    wg_add(0, 0, 768, 256, False)
    cc_send(OWN, 0)
    turn(c, e, 3)
    w_core(1)
    forward(1, 0)
    send_b(1)
    w_near(2)
    reducer(0, z_own, 0)
    flip(1, 0)
    wg_add(0, 1, 0, 256, True)
    g_in(3)
    wg_add(1, 0, 768, 256, True)
    w_core(2)
    w_core(3)
    w_core_near(0)
    w_core_near(1)
    w_near(3)
    w_core_near(2)
    reducer(0, z_own, 1)
    w_core_near(3)
    hg_other(3)
    forward(1, 1)
    x_far(1)
    g_in(1)
    hg_other(1)
    reducer(0, z_own, 2)
    hid_in(1, 1)
    hid_in(1, 2)
    flip(1, 1)
    flip(1, 2)
    wg_add(0, 1, 256, 512, False)
    g_y[2, 0].wait_recv()
    hg_other(2, 1)
    x_direct(1)
    hid_in(1, 3)
    flip(1, 3)
    wg_add(0, 1, 768, 256, False)
    cc_send(OWN, 1)
    reducer(0, z_own, 3)
    g_y[2, 1].wait_recv()
    hg_other(2, 0)
    wg_add(1, 0, 256, 512, False)
    x_summed(1)
    x_far(0)
    x_direct(0)
    wg_add(1, 1, 256, 768, True)
    reducer(1, z_own, 0)
    reducer(0, z_own, 4)
    g_in(0)
    for h in range(2):
        wg_add(1, h, 0, 256, False)
        cc_send(PAIR, h)
    reducer(1, z_own, 1)
    hg_other(0)
    z_other(0)
    reducer(1, z_own, 2)
    z_other(1)
    lo, hi = x_total(1)
    yos[:, left] = lo
    yos[:, right] = hi
    start(o_y)
    reducer(1, z_own, 3)
    z_other(2)
    x_summed(0)
    reducer(1, z_own, 4)
    z_other(3)
    z_other(4)
    lo, hi = x_total(0)
    os[:, left] = lo
    os[:, right] = hi
    put_mine = local(os, out_ref.at[:, mine], 5)
    o_y.wait_recv()

    def arrived(slot, chunks):
        for n in chunks:
            _, first, width = CHUNKS[n]
            part = yr.at[slot, :, pl.ds(first, width)]
            pltpu.make_async_copy(part, part, yrsem.at[slot, n]).wait()

    @pl.when(yh == yl)
    def _():
        arrived(0, OWN)
        arrived(1, OWN)

    @pl.when(yh != yl)
    def _():
        arrived(0, PAIR)
        arrived(1, PAIR)
        for n in OWN:
            last[n].wait_send()

    for n in PAIR:
        last[n].wait_send()
    for copy in sent:
        copy.wait_send()
    put_mine.wait()


def hand_over(
    out_ref, yr_ref, out, gq, gk, gv, out_buf, yr_buf, g_buf, into, away
):
    yr_load = pltpu.make_async_copy(yr_ref, yr_buf, into.at[4])
    yr_load.start()
    loads, stores = [], []
    for i in range(4):
        part = pl.ds(i * 32, 32)
        loads.append(pltpu.make_async_copy(out_ref.at[part], out_buf.at[part], into.at[i]))
        stores.append(pltpu.make_async_copy(out_buf.at[part], out.at[part], away.at[i]))
    for load in loads:
        load.start()
    yr_load.wait()
    g_buf[...] = yr_buf[0].astype(F32) + yr_buf[1].astype(F32)
    for i, (ref, first, width) in enumerate(((gq, 0, CQ), (gk, CQ, CK), (gv, CQ + CK, CK))):
        stores.append(pltpu.make_async_copy(g_buf.at[:, pl.ds(first, width)], ref, away.at[4 + i]))
        stores[-1].start()
    for load, store in zip(loads, stores):
        load.wait()
        store.start()
    for store in stores:
        store.wait()


N_SEM = 112


def local_step(*args):
    scratch = [
        pltpu.VMEM((2, 8, 1024, T), BF16),
        pltpu.VMEM((2, 8, T, T), BF16),
        pltpu.VMEM((1024, C), BF16),
        pltpu.VMEM((1024, C), BF16),
        pltpu.VMEM((H, 1024), BF16),
        pltpu.VMEM((H, C), BF16),
        pltpu.VMEM((C, H), BF16),
        pltpu.VMEM((512, C), BF16),
        pltpu.VMEM((1024, H), F32),
        pltpu.VMEM((2, H, C), F32),
        pltpu.VMEM((2, 1024, C), BF16),
        pltpu.VMEM((2, 1024, C), BF16),
        pltpu.VMEM((2, 3, 2, T, HH), BF16),
        pltpu.VMEM((2, 3, 2, T, HH), BF16),
        pltpu.VMEM((2, 2, 448, C), BF16),
        pltpu.VMEM((2, 2, 448, C), BF16),
        pltpu.VMEM((2, T, C), BF16),
        pltpu.VMEM((T, H), BF16),
        pltpu.VMEM((T, H), BF16),
        pltpu.SemaphoreType.DMA((11,)),
        pltpu.SemaphoreType.DMA((N_SEM,)),
        pltpu.SemaphoreType.DMA((N_SEM,)),
        pltpu.SemaphoreType.DMA((len(CHUNKS),)),
        pltpu.SemaphoreType.DMA((2, len(CHUNKS))),
    ]
    anywhere = pl.BlockSpec(memory_space=pl.ANY)
    shapes = [((T, D), BF16), ((T, CQ), F32), ((T, CK), F32), ((T, CK), F32)]
    out_shape = tuple(jax.ShapeDtypeStruct(*shape) for shape in shapes)
    terms = jax.ShapeDtypeStruct((2, T, C), BF16)
    results = pl.pallas_call(
        kernel,
        out_shape=(out_shape[0], terms),
        in_specs=[anywhere] * 7,
        out_specs=(anywhere, anywhere),
        scratch_shapes=scratch,
        compiler_params=pltpu.CompilerParams(
            collective_id=0, has_side_effects=True, vmem_limit_bytes=67043328
        ),
    )(*args)
    return pl.pallas_call(
        hand_over,
        out_shape=out_shape,
        in_specs=[anywhere] * 2,
        out_specs=(anywhere,) * 4,
        scratch_shapes=[
            pltpu.VMEM((T, D), BF16),
            pltpu.VMEM((2, T, C), BF16),
            pltpu.VMEM((T, C), F32),
            pltpu.SemaphoreType.DMA((5,)),
            pltpu.SemaphoreType.DMA((7,)),
        ],
        cost_estimate=pl.CostEstimate(flops=0, bytes_accessed=3 << 20, transcendentals=0),
    )(*results)


def solution(mesh):
    both = P(("dp", "tp"), None)
    split = P("dp", "tp")
    return jax.shard_map(
        local_step,
        mesh=mesh,
        in_specs=(both, split, split, split, P(None, "tp"), P(None, "tp"), P(None, "tp")),
        out_specs=(both, split, split, split),
        check_vma=False,
    )
```
